8 devices in a mesh: dp: 2 (over z, y), cp: 4 (over x, core).
Axes of the slice: x: 2, y: 2, z: 1, core: 2. Of those that a mesh axis runs over, the one named last changes fastest.
Arguments:
- x_in: bfloat16 [24, 768, 2048], P('dp', 'cp'), parts along dimension 0
- dy_in: bfloat16 [24, 768, 2048], P('dp', 'cp'), parts along dimension 0
- norm_gain: bfloat16 [2048], replicated
- w_q: bfloat16 [2048, 16, 128], replicated
- w_k: bfloat16 [2048, 2, 128], replicated
- w_v: bfloat16 [2048, 2, 128], replicated
- w_o: bfloat16 [16, 128, 2048], replicated
Outputs:
- output 1: bfloat16 [24, 768, 2048], P('dp', 'cp'), parts along dimension 0
- output 2: bfloat16 [24, 768, 2048], P('dp', 'cp'), parts along dimension 0
- output 3: float32 [4096], P('dp'), parts along dimension 0
- output 4: float32 [4096, 16, 128], P('dp'), parts along dimension 0
- output 5: float32 [4096, 2, 128], P('dp'), parts along dimension 0
- output 6: float32 [4096, 2, 128], P('dp'), parts along dimension 0
- output 7: float32 [32, 128, 2048], P('dp'), parts along dimension 0
There are 2 independent parts. The reference program is written for one: setup_inputs(seed, part) draws one part's arguments, and reference() takes and returns one part's arrays. A program takes and returns all parts, laid end to end along the dimension named above; an argument that names none is the same for every part.
All inputs are finite; a program needn't handle non-finite values.
Results may differ from the reference program's by a relative error of at most 0.0101.
Values are sent between devices in bfloat16 or wider.
A program may use at most 1 GiB of HBM per device.

```python
import jax
import jax.numpy as jnp
from jax import lax

BATCH_PART = 12
SEQ_LEN = 768
BLOCK_LEN = 192
MODEL_DIM = 2048
Q_HEADS = 16
KV_HEADS = 2
HEAD_DIM = 128

N_BLOCKS = SEQ_LEN // BLOCK_LEN
GROUP_SIZE = Q_HEADS // KV_HEADS
SCALE = HEAD_DIM ** -0.5
EPS = 1e-6


def setup_inputs(seed: int = 0, part: int = 0) -> dict:
    part_keys = jax.random.split(jax.random.fold_in(jax.random.key(seed), part), 2)
    weight_keys = jax.random.split(jax.random.key(seed + 1), 5)
    act_shape = (BATCH_PART, SEQ_LEN, MODEL_DIM)
    x_in = jax.random.normal(part_keys[0], act_shape, jnp.float32)
    dy_in = jax.random.normal(part_keys[1], act_shape, jnp.float32)
    norm_gain = 1.0 + 0.25 * jax.random.normal(weight_keys[0], (MODEL_DIM,), jnp.float32)
    w_q = jax.random.normal(weight_keys[1], (MODEL_DIM, Q_HEADS, HEAD_DIM), jnp.float32) * MODEL_DIM ** -0.5
    w_k = jax.random.normal(weight_keys[2], (MODEL_DIM, KV_HEADS, HEAD_DIM), jnp.float32) * MODEL_DIM ** -0.5
    w_v = jax.random.normal(weight_keys[3], (MODEL_DIM, KV_HEADS, HEAD_DIM), jnp.float32) * MODEL_DIM ** -0.5
    w_o = jax.random.normal(weight_keys[4], (Q_HEADS, HEAD_DIM, MODEL_DIM), jnp.float32) * (Q_HEADS * HEAD_DIM) ** -0.5
    return {
        'x_in': x_in.astype(jnp.bfloat16),
        'dy_in': dy_in.astype(jnp.bfloat16),
        'norm_gain': norm_gain.astype(jnp.bfloat16),
        'w_q': w_q.astype(jnp.bfloat16),
        'w_k': w_k.astype(jnp.bfloat16),
        'w_v': w_v.astype(jnp.bfloat16),
        'w_o': w_o.astype(jnp.bfloat16),
    }


def reference(x_in, dy_in, norm_gain, w_q, w_k, w_v, w_o):
    x_f32 = x_in.astype(jnp.float32)
    inv_rms = lax.rsqrt(jnp.mean(x_f32 * x_f32, axis=-1, keepdims=True) + EPS)
    unit_x = x_f32 * inv_rms
    gain_f32 = norm_gain.astype(jnp.float32)
    x_norm = (unit_x * gain_f32).astype(jnp.bfloat16)
    flat_norm = x_norm.reshape(BATCH_PART * SEQ_LEN, MODEL_DIM)
    wq_flat = w_q.reshape(MODEL_DIM, Q_HEADS * HEAD_DIM)
    wk_flat = w_k.reshape(MODEL_DIM, KV_HEADS * HEAD_DIM)
    wv_flat = w_v.reshape(MODEL_DIM, KV_HEADS * HEAD_DIM)
    wo_flat = w_o.reshape(Q_HEADS * HEAD_DIM, MODEL_DIM)
    queries = jnp.dot(flat_norm, wq_flat, preferred_element_type=jnp.float32).astype(jnp.bfloat16)
    keys_all = jnp.dot(flat_norm, wk_flat, preferred_element_type=jnp.float32).astype(jnp.bfloat16)
    values_all = jnp.dot(flat_norm, wv_flat, preferred_element_type=jnp.float32).astype(jnp.bfloat16)
    keys_f32 = keys_all.reshape(BATCH_PART, SEQ_LEN, KV_HEADS, HEAD_DIM).astype(jnp.float32)
    values_f32 = values_all.reshape(BATCH_PART, SEQ_LEN, KV_HEADS, HEAD_DIM).astype(jnp.float32)
    q_blocks = queries.reshape(BATCH_PART, N_BLOCKS, BLOCK_LEN, KV_HEADS, GROUP_SIZE, HEAD_DIM).transpose(1, 0, 2, 3, 4, 5)
    key_pos = jnp.arange(SEQ_LEN)
    block_ids = jnp.arange(N_BLOCKS)

    def block_scores(q_blk, blk_id):
        scores = jnp.einsum('bqkgd,bskd->bkgqs', q_blk.astype(jnp.float32), keys_f32) * SCALE
        query_pos = blk_id * BLOCK_LEN + jnp.arange(BLOCK_LEN)
        visible = query_pos[:, None] >= key_pos[None, :]
        return scores, visible

    def forward_block(operands):
        q_blk, blk_id = operands
        scores, visible = block_scores(q_blk, blk_id)
        scores = jnp.where(visible, scores, -jnp.inf)
        row_max = jnp.max(scores, axis=-1)
        probs_raw = jnp.exp(scores - row_max[..., None])
        row_sum = jnp.sum(probs_raw, axis=-1)
        attn_blk = jnp.einsum('bkgqs,bskd->bkgqd', probs_raw.astype(jnp.bfloat16).astype(jnp.float32), values_f32) / row_sum[..., None]
        return attn_blk.astype(jnp.bfloat16), row_max + jnp.log(row_sum)

    attn_blocks, log_norm = lax.map(forward_block, (q_blocks, block_ids))
    attn_tok = attn_blocks.transpose(1, 0, 4, 2, 3, 5).reshape(BATCH_PART * SEQ_LEN, Q_HEADS * HEAD_DIM)
    proj_out = jnp.dot(attn_tok, wo_flat, preferred_element_type=jnp.float32)
    y_out = (x_f32 + proj_out.reshape(BATCH_PART, SEQ_LEN, MODEL_DIM)).astype(jnp.bfloat16)

    dy_flat = dy_in.reshape(BATCH_PART * SEQ_LEN, MODEL_DIM)
    d_wo = jnp.dot(attn_tok.T, dy_flat, preferred_element_type=jnp.float32).reshape(Q_HEADS, HEAD_DIM, MODEL_DIM)
    d_attn = jnp.dot(dy_flat, wo_flat.T, preferred_element_type=jnp.float32).astype(jnp.bfloat16)
    d_attn_blocks = d_attn.reshape(BATCH_PART, N_BLOCKS, BLOCK_LEN, KV_HEADS, GROUP_SIZE, HEAD_DIM).transpose(1, 0, 3, 4, 2, 5)
    delta_row = jnp.sum(d_attn_blocks.astype(jnp.float32) * attn_blocks.astype(jnp.float32), axis=-1)

    def backward_block(grad_carry, operands):
        d_keys, d_values = grad_carry
        q_blk, blk_id, d_attn_blk, delta_blk, log_blk = operands
        scores, visible = block_scores(q_blk, blk_id)
        probs_norm = jnp.where(visible, jnp.exp(scores - log_blk[..., None]), 0.0)
        d_attn_f32 = d_attn_blk.astype(jnp.float32)
        d_values = d_values + jnp.einsum('bkgqs,bkgqd->bskd', probs_norm.astype(jnp.bfloat16).astype(jnp.float32), d_attn_f32)
        d_probs = jnp.einsum('bkgqd,bskd->bkgqs', d_attn_f32, values_f32)
        d_scores = (probs_norm * (d_probs - delta_blk[..., None]) * SCALE).astype(jnp.bfloat16).astype(jnp.float32)
        d_query = jnp.einsum('bkgqs,bskd->bqkgd', d_scores, keys_f32)
        d_keys = d_keys + jnp.einsum('bkgqs,bqkgd->bskd', d_scores, q_blk.astype(jnp.float32))
        return (d_keys, d_values), d_query

    zero_kv = jnp.zeros((BATCH_PART, SEQ_LEN, KV_HEADS, HEAD_DIM), jnp.float32)
    grad_kv, d_query_blocks = lax.scan(backward_block, (zero_kv, zero_kv), (q_blocks, block_ids, d_attn_blocks, delta_row, log_norm))
    d_query = d_query_blocks.transpose(1, 0, 2, 3, 4, 5).reshape(BATCH_PART * SEQ_LEN, Q_HEADS * HEAD_DIM).astype(jnp.bfloat16)
    d_keys = grad_kv[0].reshape(BATCH_PART * SEQ_LEN, KV_HEADS * HEAD_DIM).astype(jnp.bfloat16)
    d_values = grad_kv[1].reshape(BATCH_PART * SEQ_LEN, KV_HEADS * HEAD_DIM).astype(jnp.bfloat16)
    d_wq = jnp.dot(flat_norm.T, d_query, preferred_element_type=jnp.float32).reshape(MODEL_DIM, Q_HEADS, HEAD_DIM)
    d_wk = jnp.dot(flat_norm.T, d_keys, preferred_element_type=jnp.float32).reshape(MODEL_DIM, KV_HEADS, HEAD_DIM)
    d_wv = jnp.dot(flat_norm.T, d_values, preferred_element_type=jnp.float32).reshape(MODEL_DIM, KV_HEADS, HEAD_DIM)
    d_norm = (jnp.dot(d_query, wq_flat.T, preferred_element_type=jnp.float32)
              + jnp.dot(d_keys, wk_flat.T, preferred_element_type=jnp.float32)
              + jnp.dot(d_values, wv_flat.T, preferred_element_type=jnp.float32)).reshape(BATCH_PART, SEQ_LEN, MODEL_DIM)
    d_gain = jnp.sum(d_norm * unit_x, axis=(0, 1))
    d_unit = d_norm * gain_f32
    d_x = inv_rms * (d_unit - unit_x * jnp.mean(d_unit * unit_x, axis=-1, keepdims=True))
    dx_out = (dy_in.astype(jnp.float32) + d_x).astype(jnp.bfloat16)
    return y_out, dx_out, d_gain, d_wq, d_wk, d_wv, d_wo
```

```python
import functools

import jax
import jax.numpy as jnp
from jax import lax
from jax.experimental import pallas as pl
from jax.experimental.pallas import tpu as pltpu
from jax.sharding import PartitionSpec as P

EPS = 1e-6
F32 = jnp.float32
BF16 = jnp.bfloat16
LOG2E = 1.4426950408889634
MESH = pl.DeviceIdType.MESH
CROSS_AHEAD = 4
PAIR_AHEAD = 2


def dot_nn(a, b):
    return lax.dot_general(a, b, (((1,), (0,)), ((), ())), preferred_element_type=F32)


def dot_nt(a, b):
    return lax.dot_general(a, b, (((1,), (1,)), ((), ())), preferred_element_type=F32)


def group_kernel(xn, dy, wqkv, wo, gx, gy, dwo, dwq, oo, dqo,
                 xb, yb, wq_v, wo_v, acc_o, acc_q, q_s, do_s, k_s, v_s, kt_s, vt_s,
                 ot_s, dqt_s, dk_acc, dv_acc, o_n, dq_n,
                 cs, cr, ds, dr, fs, fr, lsem, wsem, osem, psend, precv, fsem):
    n_seq, blk, dm = xn.shape
    seq = 4 * blk
    n_heads, _, hd = q_s.shape
    qw = n_heads * hd
    half = 2 * blk
    tile = 256
    n_tiles = seq // tile
    c2 = LOG2E * hd ** -0.5
    scale = hd ** -0.5

    me = lax.axis_index('cp')
    core = me % 2
    chip = me // 2
    pair = chip * 2 + (1 - core)
    across = (1 - chip) * 2 + core
    diag = (1 - chip) * 2 + (1 - core)
    src_of = (xn, dy)
    land_of = (gx, gy)
    vmem_of = (xb, yb)

    def cross_copy(t, s):
        return pltpu.make_async_remote_copy(src_of[t].at[s], land_of[t].at[me, s], cs.at[t, s], cr.at[t, s],
                                            device_id={'cp': across}, device_id_type=MESH)

    def cross_arrival(t, s):
        return pltpu.make_async_remote_copy(src_of[t].at[s], land_of[t].at[across, s], cs.at[t, s], cr.at[t, s],
                                            device_id={'cp': across}, device_id_type=MESH)

    def pair_copy(t, s):
        return pltpu.make_async_remote_copy(src_of[t].at[s], land_of[t].at[me, s], ds.at[t, s], dr.at[t, s],
                                            device_id={'cp': pair}, device_id_type=MESH)

    def pair_arrival(t, s):
        return pltpu.make_async_remote_copy(src_of[t].at[s], land_of[t].at[pair, s], ds.at[t, s], dr.at[t, s],
                                            device_id={'cp': pair}, device_id_type=MESH)

    def fwd_copy(t, s):
        return pltpu.make_async_remote_copy(land_of[t].at[across, s], land_of[t].at[across, s], fs.at[t, s], fr.at[t, s],
                                            device_id={'cp': pair}, device_id_type=MESH)

    def fwd_arrival(t, s):
        return pltpu.make_async_remote_copy(land_of[t].at[across, s], land_of[t].at[diag, s], fs.at[t, s], fr.at[t, s],
                                            device_id={'cp': pair}, device_id_type=MESH)

    def rows_of(b):
        return pl.ds(pl.multiple_of(b * blk, 64), blk)

    def load_own(t, s):
        return pltpu.make_async_copy(src_of[t].at[s], vmem_of[t].at[s % 2, rows_of(me)], lsem.at[t, 0])

    def load_from(t, s, b, j):
        return pltpu.make_async_copy(land_of[t].at[b, s], vmem_of[t].at[s % 2, rows_of(b)], lsem.at[t, j])

    def out_copies(s):
        own_rows = pl.ds(pl.multiple_of(core * blk, 64), blk)
        pair_rows = pl.ds(pl.multiple_of((1 - core) * blk, 64), blk)
        res = []
        for idx, (buf, out) in enumerate(((o_n, oo), (dq_n, dqo))):
            width = buf.shape[1]
            cols = pl.ds(pl.multiple_of(core * width, 128), width)
            res.append((pltpu.make_async_copy(buf.at[own_rows], out.at[s, :, cols], osem.at[idx]),
                        pltpu.make_async_remote_copy(buf.at[pair_rows], out.at[s, :, cols], psend.at[idx], precv.at[idx, s],
                                                     device_id={'cp': pair}, device_id_type=MESH)))
        return res

    def out_arrivals(s):
        pair_rows = pl.ds(pl.multiple_of((1 - core) * blk, 64), blk)
        res = []
        for idx, (buf, out) in enumerate(((o_n, oo), (dq_n, dqo))):
            width = buf.shape[1]
            cols = pl.ds(pl.multiple_of((1 - core) * width, 128), width)
            res.append(pltpu.make_async_remote_copy(buf.at[pair_rows], out.at[s, :, cols], psend.at[idx], precv.at[idx, s],
                                                    device_id={'cp': pair}, device_id_type=MESH))
        return res

    load_wq = pltpu.make_async_copy(wqkv, wq_v, wsem.at[0])
    load_wo = pltpu.make_async_copy(wo, wo_v, wsem.at[1])
    load_wq.start()
    load_wo.start()

    barrier = pltpu.get_barrier_semaphore()
    for peer in (pair, across):
        pl.semaphore_signal(barrier, inc=1, device_id={'cp': peer}, device_id_type=MESH)
    pl.semaphore_wait(barrier, 2)

    for s in range(CROSS_AHEAD):
        for t in range(2):
            cross_copy(t, s).start()
            if s < PAIR_AHEAD:
                pair_copy(t, s).start()
    for t in range(2):
        load_own(t, 0).start()
    acc_o[...] = jnp.zeros_like(acc_o)
    acc_q[...] = jnp.zeros_like(acc_q)
    for t in range(2):
        pair_arrival(t, 0).wait_recv()
        load_from(t, 0, pair, 1).start()
    load_wq.wait()
    load_wo.wait()

    def project_x(slot, r0):
        rows = pl.ds(pl.multiple_of(r0, 128), half)
        for n in range((qw + 2 * hd) // tile):
            res = dot_nn(xb[slot, rows, :], wq_v[:, n * tile:(n + 1) * tile]).astype(BF16)
            for part in range(tile // hd):
                col = n * tile + part * hd
                piece = res[:, part * hd:(part + 1) * hd]
                if col < qw:
                    q_s[col // hd, rows, :] = piece
                elif col == qw:
                    k_s[rows, :] = piece
                else:
                    v_s[rows, :] = piece

    def project_dy(slot, r0):
        rows = pl.ds(pl.multiple_of(r0, 128), half)
        for n in range(qw // tile):
            res = dot_nt(yb[slot, rows, :], wo_v[n * tile:(n + 1) * tile, :]).astype(BF16)
            for part in range(tile // hd):
                do_s[(n * tile + part * hd) // hd, rows, :] = res[:, part * hd:(part + 1) * hd]

    def head_step(h, carry):
        hrows = pl.ds(pl.multiple_of(h * hd, hd), hd)
        for i in range(n_tiles):
            nk = (i + 1) * tile
            qi = q_s[h, i * tile:(i + 1) * tile, :]
            doi = do_s[h, i * tile:(i + 1) * tile, :]
            st = dot_nt(k_s[0:nk, :], qi)
            key_pos = lax.broadcasted_iota(jnp.int32, (nk, tile), 0)
            qry_pos = lax.broadcasted_iota(jnp.int32, (nk, tile), 1) + i * tile
            st = jnp.where(key_pos <= qry_pos, st, -jnp.inf)
            mx = jnp.max(st, axis=0, keepdims=True)
            p = jnp.exp2(st * c2 - mx * c2)
            inv_l = 1.0 / jnp.sum(p, axis=0, keepdims=True)
            ot = (dot_nn(vt_s[:, 0:nk], p.astype(BF16)) * inv_l).astype(BF16)
            ot_s[hrows, i * tile:(i + 1) * tile] = ot
            dot_i = doi.astype(F32).T
            delta = jnp.sum(dot_i * ot.astype(F32), axis=0, keepdims=True)
            dpt = dot_nt(v_s[0:nk, :], doi)
            pn = p * inv_l
            dst = (pn * (dpt - delta) * scale).astype(BF16)
            dv_acc[0:nk, :] += dot_nn(pn.astype(BF16), doi)
            dk_acc[0:nk, :] += dot_nn(dst, qi)
            dqt_s[hrows, i * tile:(i + 1) * tile] = dot_nn(kt_s[:, 0:nk], dst).astype(BF16)
        own_cols = pl.ds(pl.multiple_of(chip * half, 128), half)
        hcols = pl.ds(pl.multiple_of(h * hd, hd), hd)
        o_n[:, hcols] = ot_s[hrows, own_cols].T
        dq_n[:, hcols] = dqt_s[hrows, own_cols].T
        return carry

    def seq_step(s, carry):
        slot = s % 2
        @pl.when(s + CROSS_AHEAD < n_seq)
        def _():
            for t in range(2):
                cross_copy(t, s + CROSS_AHEAD).start()
        @pl.when(s + PAIR_AHEAD < n_seq)
        def _():
            for t in range(2):
                pair_copy(t, s + PAIR_AHEAD).start()

        cross_arrival(0, s).wait_recv()
        fwd_copy(0, s).start()
        load_from(0, s, across, 2).start()
        for t in range(2):
            load_own(t, s).wait()
            load_from(t, s, pair, 1).wait()
        near = chip * half
        far = (1 - chip) * half
        project_x(slot, near)
        project_dy(slot, near)
        fwd_arrival(0, s).wait_recv()
        load_from(0, s, diag, 3).start()
        load_from(0, s, across, 2).wait()
        load_from(0, s, diag, 3).wait()
        project_x(slot, far)
        cross_arrival(1, s).wait_recv()
        fwd_copy(1, s).start()
        load_from(1, s, across, 2).start()
        fwd_arrival(1, s).wait_recv()
        load_from(1, s, diag, 3).start()

        kt_s[...] = k_s[...].T
        vt_s[...] = v_s[...].T
        dk_acc[...] = jnp.zeros_like(dk_acc)
        dv_acc[...] = jnp.zeros_like(dv_acc)
        load_from(1, s, across, 2).wait()
        load_from(1, s, diag, 3).wait()
        project_dy(slot, far)

        @pl.when(s + 1 < n_seq)
        def _():
            for t in range(2):
                load_own(t, s + 1).start()
                pair_arrival(t, s + 1).wait_recv()
                load_from(t, s + 1, pair, 1).start()

        @pl.when(s > 0)
        def _():
            for local, remote in out_copies(s - 1):
                local.wait()
                remote.wait_send()

        lax.fori_loop(0, n_heads, head_step, 0)

        near_rows = pl.ds(pl.multiple_of(near, 128), half)
        for idx, acc in enumerate((dk_acc, dv_acc)):
            lo = qw + idx * hd
            dqt_s[lo:lo + hd, :] = acc[...].T.astype(BF16)
            dq_n[:, lo:lo + hd] = acc[near_rows, :].astype(BF16)
        for local, remote in out_copies(s):
            local.start()
            remote.start()

        def dw_step(n, c):
            cols = pl.ds(pl.multiple_of(n * 2 * tile, 2 * tile), 2 * tile)
            acc_o[:, cols] += dot_nn(ot_s[...], yb[slot, :, cols])
            acc_q[:, cols] += dot_nn(dqt_s[...], xb[slot, :, cols])
            return c

        lax.fori_loop(0, dm // (2 * tile), dw_step, 0)
        return carry

    lax.fori_loop(0, n_seq, seq_step, 0)

    flush_o = pltpu.make_async_copy(acc_o, dwo, fsem.at[0])
    flush_q = pltpu.make_async_copy(acc_q, dwq, fsem.at[1])
    flush_o.start()
    flush_q.start()
    for local, remote in out_copies(n_seq - 1):
        local.wait()
        remote.wait_send()

    def drain(s, carry):
        for t in range(2):
            cross_copy(t, s).wait_send()
            pair_copy(t, s).wait_send()
            fwd_copy(t, s).wait_send()
        for arrival in out_arrivals(s):
            arrival.wait_recv()
        return carry

    lax.fori_loop(0, n_seq, drain, 0)
    flush_o.wait()
    flush_q.wait()


def group_call(x_norm, dy_in, wqkv, wo):
    n_seq, blk, dm = x_norm.shape
    seq = 4 * blk
    qw = wo.shape[0]
    hd = (wqkv.shape[1] - qw) // 2
    n_heads = qw // hd
    kw = wqkv.shape[1]
    any_spec = pl.BlockSpec(memory_space=pl.ANY)
    dma = pltpu.SemaphoreType.DMA
    return pl.pallas_call(
        group_kernel,
        out_shape=(
            jax.ShapeDtypeStruct((4, n_seq, blk, dm), BF16),
            jax.ShapeDtypeStruct((4, n_seq, blk, dm), BF16),
            jax.ShapeDtypeStruct((qw, dm), F32),
            jax.ShapeDtypeStruct((kw, dm), F32),
            jax.ShapeDtypeStruct((n_seq, blk, 2 * qw), BF16),
            jax.ShapeDtypeStruct((n_seq, blk, 2 * kw), BF16),
        ),
        in_specs=[any_spec] * 4,
        out_specs=(any_spec,) * 6,
        scratch_shapes=[
            pltpu.VMEM((2, seq, dm), BF16), pltpu.VMEM((2, seq, dm), BF16),
            pltpu.VMEM((dm, kw), BF16), pltpu.VMEM((qw, dm), BF16),
            pltpu.VMEM((qw, dm), F32), pltpu.VMEM((kw, dm), F32),
            pltpu.VMEM((n_heads, seq, hd), BF16), pltpu.VMEM((n_heads, seq, hd), BF16),
            pltpu.VMEM((seq, hd), BF16), pltpu.VMEM((seq, hd), BF16),
            pltpu.VMEM((hd, seq), BF16), pltpu.VMEM((hd, seq), BF16),
            pltpu.VMEM((qw, seq), BF16), pltpu.VMEM((kw, seq), BF16),
            pltpu.VMEM((seq, hd), F32), pltpu.VMEM((seq, hd), F32),
            pltpu.VMEM((2 * blk, qw), BF16), pltpu.VMEM((2 * blk, kw), BF16),
            dma((2, n_seq)), dma((2, n_seq)), dma((2, n_seq)), dma((2, n_seq)), dma((2, n_seq)), dma((2, n_seq)),
            dma((2, 4)), dma((2,)), dma((2,)), dma((2,)), dma((2, n_seq)), dma((2,)),
        ],
        compiler_params=pltpu.CompilerParams(collective_id=0, has_side_effects=True, vmem_limit_bytes=67_000_000),
    )(x_norm, dy_in, wqkv, wo)


def solution(mesh):
    def device_fn(x_in, dy_in, norm_gain, w_q, w_k, w_v, w_o):
        n_batch, blk, dm = x_in.shape
        n_heads, hd = w_q.shape[1], w_q.shape[2]
        kv_heads = w_k.shape[1]
        n_group = n_heads // kv_heads
        core = lax.axis_index('cp') % 2
        gain = norm_gain.astype(F32)
        x_f32 = x_in.astype(F32)
        inv_rms = lax.rsqrt(jnp.mean(x_f32 * x_f32, axis=-1, keepdims=True) + EPS)
        unit = x_f32 * inv_rms
        x_norm = (unit * gain).astype(BF16)

        w_all = jnp.concatenate(
            [part for g in range(kv_heads) for part in
             (w_q[:, g * n_group:(g + 1) * n_group].reshape(dm, n_group * hd), w_k[:, g], w_v[:, g])], axis=1)
        kw = w_all.shape[1] // kv_heads
        wqkv = lax.dynamic_slice(w_all, (0, core * kw), (dm, kw))
        wo_all = w_o.reshape(n_heads * hd, dm)
        wo = lax.dynamic_slice(wo_all, (core * n_group * hd, 0), (n_group * hd, dm))

        _, _, dwo_half, dwq_half, o_own, dq_own = group_call(x_norm, dy_in, wqkv, wo)

        pairs = [[0, 1], [2, 3]]
        d_wo = lax.all_gather(dwo_half, 'cp', axis_index_groups=pairs, tiled=True).reshape(n_heads, hd, dm)
        dwq_all = lax.all_gather(dwq_half, 'cp', axis_index_groups=pairs)
        qw = n_group * hd
        d_wq = dwq_all[:, :qw].reshape(n_heads, hd, dm).transpose(2, 0, 1)
        d_wk = dwq_all[:, qw:qw + hd].transpose(2, 0, 1)
        d_wv = dwq_all[:, qw + hd:].transpose(2, 0, 1)

        y_out = (x_f32 + jnp.einsum('bsf,fm->bsm', o_own, wo_all, preferred_element_type=F32)).astype(BF16)
        d_norm = jnp.einsum('bsf,mf->bsm', dq_own, w_all, preferred_element_type=F32)
        d_gain = lax.psum(jnp.sum(d_norm * unit, axis=(0, 1)), 'cp')
        d_unit = d_norm * gain
        dx_out = (dy_in.astype(F32) + inv_rms * (d_unit - unit * jnp.mean(d_unit * unit, axis=-1, keepdims=True))).astype(BF16)
        return y_out, dx_out, d_gain, d_wq, d_wk, d_wv, d_wo

    act_spec = P('dp', 'cp', None)
    mat_spec = P(None, None, None)
    grad_spec = P('dp', None, None)
    return jax.shard_map(device_fn, mesh=mesh,
                         in_specs=(act_spec, act_spec, P(None), mat_spec, mat_spec, mat_spec, mat_spec),
                         out_specs=(act_spec, act_spec, P('dp'), grad_spec, grad_spec, grad_spec, grad_spec),
                         check_vma=False)
```

```python
import functools

import jax
import jax.numpy as jnp
from jax import lax
from jax.experimental import pallas as pl
from jax.experimental.pallas import tpu as pltpu
from jax.sharding import PartitionSpec as P

EPS = 1e-6
F32 = jnp.float32
BF16 = jnp.bfloat16
LOG2E = 1.4426950408889634
MESH = pl.DeviceIdType.MESH
CROSS_AHEAD = 4
PAIR_AHEAD = 2


def dot_nn(a, b):
    return lax.dot_general(a, b, (((1,), (0,)), ((), ())), preferred_element_type=F32)


def dot_nt(a, b):
    return lax.dot_general(a, b, (((1,), (1,)), ((), ())), preferred_element_type=F32)


def group_kernel(x, dy, gain, wq, wkv, wo, gx, gy, dwo, dwq, oo, dqo, xn,
                 xb, yb, gain_v, wq_v, wo_v, acc_o, acc_q, q_s, do_s, k_s, v_s, kt_s, vt_s,
                 ot_s, dqt_s, dk_acc, dv_acc, o_n, dq_n,
                 cs, cr, ds, dr, fs, fr, lsem, wsem, osem, psend, precv, fsem, nsem):
    n_seq, blk, dm = x.shape
    seq = 4 * blk
    n_heads, _, hd = q_s.shape
    qw = n_heads * hd
    half = 2 * blk
    tile = 256
    n_tiles = seq // tile
    c2 = LOG2E * hd ** -0.5
    scale = hd ** -0.5

    me = lax.axis_index('cp')
    core = me % 2
    chip = me // 2
    pair = chip * 2 + (1 - core)
    across = (1 - chip) * 2 + core
    diag = (1 - chip) * 2 + (1 - core)
    src_of = (xn, dy)
    land_of = (gx, gy)
    vmem_of = (xb, yb)

    def cross_copy(t, s):
        return pltpu.make_async_remote_copy(src_of[t].at[s], land_of[t].at[me, s], cs.at[t, s], cr.at[t, s],
                                            device_id={'cp': across}, device_id_type=MESH)

    def cross_arrival(t, s):
        return pltpu.make_async_remote_copy(src_of[t].at[s], land_of[t].at[across, s], cs.at[t, s], cr.at[t, s],
                                            device_id={'cp': across}, device_id_type=MESH)

    def pair_copy(t, s):
        return pltpu.make_async_remote_copy(src_of[t].at[s], land_of[t].at[me, s], ds.at[t, s], dr.at[t, s],
                                            device_id={'cp': pair}, device_id_type=MESH)

    def pair_arrival(t, s):
        return pltpu.make_async_remote_copy(src_of[t].at[s], land_of[t].at[pair, s], ds.at[t, s], dr.at[t, s],
                                            device_id={'cp': pair}, device_id_type=MESH)

    def fwd_copy(t, s):
        return pltpu.make_async_remote_copy(land_of[t].at[across, s], land_of[t].at[across, s], fs.at[t, s], fr.at[t, s],
                                            device_id={'cp': pair}, device_id_type=MESH)

    def fwd_arrival(t, s):
        return pltpu.make_async_remote_copy(land_of[t].at[across, s], land_of[t].at[diag, s], fs.at[t, s], fr.at[t, s],
                                            device_id={'cp': pair}, device_id_type=MESH)

    def rows_of(b):
        return pl.ds(pl.multiple_of(b * blk, 64), blk)

    def load_own(t, s):
        return pltpu.make_async_copy(src_of[t].at[s], vmem_of[t].at[s % 2, rows_of(me)], lsem.at[t, 0])

    def load_from(t, s, b, j):
        return pltpu.make_async_copy(land_of[t].at[b, s], vmem_of[t].at[s % 2, rows_of(b)], lsem.at[t, j])

    def out_copies(s):
        own_rows = pl.ds(pl.multiple_of(core * blk, 64), blk)
        pair_rows = pl.ds(pl.multiple_of((1 - core) * blk, 64), blk)
        res = []
        for idx, (buf, out) in enumerate(((o_n, oo), (dq_n, dqo))):
            width = buf.shape[1]
            cols = pl.ds(pl.multiple_of(core * width, 128), width)
            res.append((pltpu.make_async_copy(buf.at[own_rows], out.at[s, :, cols], osem.at[idx]),
                        pltpu.make_async_remote_copy(buf.at[pair_rows], out.at[s, :, cols], psend.at[idx], precv.at[idx, s],
                                                     device_id={'cp': pair}, device_id_type=MESH)))
        return res

    def out_arrivals(s):
        pair_rows = pl.ds(pl.multiple_of((1 - core) * blk, 64), blk)
        res = []
        for idx, (buf, out) in enumerate(((o_n, oo), (dq_n, dqo))):
            width = buf.shape[1]
            cols = pl.ds(pl.multiple_of((1 - core) * width, 128), width)
            res.append(pltpu.make_async_remote_copy(buf.at[pair_rows], out.at[s, :, cols], psend.at[idx], precv.at[idx, s],
                                                    device_id={'cp': pair}, device_id_type=MESH))
        return res

    kvw = 2 * hd
    weight_loads = [
        pltpu.make_async_copy(gain, gain_v, wsem.at[0]),
        pltpu.make_async_copy(wq.at[:, pl.ds(pl.multiple_of(core * qw, 128), qw)], wq_v.at[:, 0:qw], wsem.at[1]),
        pltpu.make_async_copy(wkv.at[:, pl.ds(pl.multiple_of(core * kvw, 128), kvw)], wq_v.at[:, qw:qw + kvw], wsem.at[2]),
        pltpu.make_async_copy(wo.at[pl.ds(pl.multiple_of(core * qw, 128), qw)], wo_v, wsem.at[3]),
    ]

    def norm_in(s):
        return pltpu.make_async_copy(x.at[s], yb.at[1, pl.ds(pl.multiple_of((s % 2) * blk, 64), blk)], nsem.at[0, s % 2])

    def norm_out(s):
        return pltpu.make_async_copy(xb.at[1, pl.ds(pl.multiple_of((s % 2) * blk, 64), blk)], xn.at[s], nsem.at[1, s % 2])

    norm_in(0).start()
    for copy in weight_loads:
        copy.start()

    barrier = pltpu.get_barrier_semaphore()
    for peer in (pair, across):
        pl.semaphore_signal(barrier, inc=1, device_id={'cp': peer}, device_id_type=MESH)
    pl.semaphore_wait(barrier, 2)

    cross_copy(1, 0).start()
    pair_copy(1, 0).start()
    load_own(1, 0).start()
    weight_loads[0].wait()

    def send_normed(s):
        norm_out(s).wait()

        @pl.when(s < CROSS_AHEAD)
        def _():
            cross_copy(0, s).start()

        @pl.when(s + 1 < CROSS_AHEAD)
        def _():
            cross_copy(1, s + 1).start()

        @pl.when(s < PAIR_AHEAD)
        def _():
            pair_copy(0, s).start()

        @pl.when(s + 1 < PAIR_AHEAD)
        def _():
            pair_copy(1, s + 1).start()

    def norm_step(s, carry):
        @pl.when(s + 1 < n_seq)
        def _():
            norm_in(s + 1).start()
        norm_in(s).wait()
        base = (s % 2) * blk
        for c in range(blk // 48):
            rows = pl.ds(pl.multiple_of(base + c * 48, 16), 48)
            xf = yb[1, rows, :].astype(F32)
            r = lax.rsqrt(jnp.mean(xf * xf, axis=-1, keepdims=True) + EPS)
            xb[1, rows, :] = (xf * r * gain_v[...]).astype(BF16)
        norm_out(s).start()

        @pl.when(s > 0)
        def _():
            send_normed(s - 1)
        return carry

    lax.fori_loop(0, n_seq, norm_step, 0)
    send_normed(n_seq - 1)
    load_own(0, 0).start()
    acc_o[...] = jnp.zeros_like(acc_o)
    acc_q[...] = jnp.zeros_like(acc_q)
    for t in range(2):
        pair_arrival(t, 0).wait_recv()
        load_from(t, 0, pair, 1).start()
    for copy in weight_loads[1:]:
        copy.wait()

    def project_x(slot, r0):
        rows = pl.ds(pl.multiple_of(r0, 128), half)
        for n in range((qw + 2 * hd) // tile):
            res = dot_nn(xb[slot, rows, :], wq_v[:, n * tile:(n + 1) * tile]).astype(BF16)
            for part in range(tile // hd):
                col = n * tile + part * hd
                piece = res[:, part * hd:(part + 1) * hd]
                if col < qw:
                    q_s[col // hd, rows, :] = piece
                elif col == qw:
                    k_s[rows, :] = piece
                else:
                    v_s[rows, :] = piece

    def project_dy(slot, r0):
        rows = pl.ds(pl.multiple_of(r0, 128), half)
        for n in range(qw // tile):
            res = dot_nt(yb[slot, rows, :], wo_v[n * tile:(n + 1) * tile, :]).astype(BF16)
            for part in range(tile // hd):
                do_s[(n * tile + part * hd) // hd, rows, :] = res[:, part * hd:(part + 1) * hd]

    def heads():
        units = [(h, i) for h in range(n_heads) for i in range(n_tiles)]
        state = {}

        def score(u):
            h, i = units[u]
            nk = (i + 1) * tile
            qi = q_s[h, i * tile:(i + 1) * tile, :]
            doi = do_s[h, i * tile:(i + 1) * tile, :]
            state[u] = [dot_nt(k_s[0:nk, :], qi), dot_nt(v_s[0:nk, :], doi)]

        def attend(u):
            h, i = units[u]
            nk = (i + 1) * tile
            st, dpt = state[u]
            key_pos = lax.broadcasted_iota(jnp.int32, (tile, tile), 0)
            qry_pos = lax.broadcasted_iota(jnp.int32, (tile, tile), 1)
            edge = jnp.where(key_pos <= qry_pos, st[nk - tile:], -jnp.inf)
            st = edge if i == 0 else jnp.concatenate([st[:nk - tile], edge], axis=0)
            mx = jnp.max(st, axis=0, keepdims=True)
            p = jnp.exp2(st * c2 - mx * c2)
            inv_l = 1.0 / jnp.sum(p, axis=0, keepdims=True)
            ot = (dot_nn(vt_s[:, 0:nk], p.astype(BF16)) * inv_l).astype(BF16)
            ot_s[h * hd:(h + 1) * hd, i * tile:(i + 1) * tile] = ot
            state[u] = [p, inv_l, ot, dpt]

        def grads(u):
            h, i = units[u]
            nk = (i + 1) * tile
            p, inv_l, ot, dpt = state.pop(u)
            qi = q_s[h, i * tile:(i + 1) * tile, :]
            doi = do_s[h, i * tile:(i + 1) * tile, :]
            delta = jnp.sum(doi.astype(F32).T * ot.astype(F32), axis=0, keepdims=True)
            pn = p * inv_l
            dst = (pn * (dpt - delta) * scale).astype(BF16)
            dv_acc[0:nk, :] += dot_nn(pn.astype(BF16), doi)
            dk_acc[0:nk, :] += dot_nn(dst, qi)
            dqt_s[h * hd:(h + 1) * hd, i * tile:(i + 1) * tile] = dot_nn(kt_s[:, 0:nk], dst).astype(BF16)

        for t in range(-2, len(units)):
            if t + 2 < len(units):
                score(t + 2)
            if 0 <= t + 1 < len(units):
                attend(t + 1)
            if t >= 0:
                grads(t)
        own_cols = pl.ds(pl.multiple_of(chip * half, 128), half)
        for h in range(n_heads):
            o_n[:, h * hd:(h + 1) * hd] = ot_s[h * hd:(h + 1) * hd, own_cols].T
            dq_n[:, h * hd:(h + 1) * hd] = dqt_s[h * hd:(h + 1) * hd, own_cols].T

    def seq_step(s, carry):
        slot = s % 2
        @pl.when(s + CROSS_AHEAD < n_seq)
        def _():
            for t in range(2):
                cross_copy(t, s + CROSS_AHEAD).start()
        @pl.when(s + PAIR_AHEAD < n_seq)
        def _():
            for t in range(2):
                pair_copy(t, s + PAIR_AHEAD).start()

        cross_arrival(0, s).wait_recv()
        fwd_copy(0, s).start()
        load_from(0, s, across, 2).start()
        for t in range(2):
            load_own(t, s).wait()
            load_from(t, s, pair, 1).wait()
        near = chip * half
        far = (1 - chip) * half
        project_x(slot, near)
        project_dy(slot, near)
        fwd_arrival(0, s).wait_recv()
        load_from(0, s, diag, 3).start()
        load_from(0, s, across, 2).wait()
        load_from(0, s, diag, 3).wait()
        project_x(slot, far)
        cross_arrival(1, s).wait_recv()
        fwd_copy(1, s).start()
        load_from(1, s, across, 2).start()
        fwd_arrival(1, s).wait_recv()
        load_from(1, s, diag, 3).start()

        kt_s[...] = k_s[...].T
        vt_s[...] = v_s[...].T
        dk_acc[...] = jnp.zeros_like(dk_acc)
        dv_acc[...] = jnp.zeros_like(dv_acc)
        load_from(1, s, across, 2).wait()
        load_from(1, s, diag, 3).wait()
        project_dy(slot, far)

        @pl.when(s + 1 < n_seq)
        def _():
            for t in range(2):
                load_own(t, s + 1).start()
                pair_arrival(t, s + 1).wait_recv()
                load_from(t, s + 1, pair, 1).start()

        @pl.when(s > 0)
        def _():
            for local, remote in out_copies(s - 1):
                local.wait()
                remote.wait_send()

        heads()

        near_rows = pl.ds(pl.multiple_of(near, 128), half)
        for idx, acc in enumerate((dk_acc, dv_acc)):
            lo = qw + idx * hd
            dqt_s[lo:lo + hd, :] = acc[...].T.astype(BF16)
            dq_n[:, lo:lo + hd] = acc[near_rows, :].astype(BF16)
        for local, remote in out_copies(s):
            local.start()
            remote.start()

        def dw_step(n, c):
            cols = pl.ds(pl.multiple_of(n * 2 * tile, 2 * tile), 2 * tile)
            acc_o[:, cols] += dot_nn(ot_s[...], yb[slot, :, cols])
            acc_q[:, cols] += dot_nn(dqt_s[...], xb[slot, :, cols])
            return c

        lax.fori_loop(0, dm // (2 * tile), dw_step, 0)
        return carry

    lax.fori_loop(0, n_seq, seq_step, 0)

    flush_o = pltpu.make_async_copy(acc_o, dwo, fsem.at[0])
    flush_q = pltpu.make_async_copy(acc_q, dwq, fsem.at[1])
    flush_o.start()
    flush_q.start()
    for local, remote in out_copies(n_seq - 1):
        local.wait()
        remote.wait_send()

    def drain(s, carry):
        for t in range(2):
            cross_copy(t, s).wait_send()
            pair_copy(t, s).wait_send()
            fwd_copy(t, s).wait_send()
        for arrival in out_arrivals(s):
            arrival.wait_recv()
        return carry

    lax.fori_loop(0, n_seq, drain, 0)
    flush_o.wait()
    flush_q.wait()


def group_call(x_in, dy_in, gain, wq, wkv, wo):
    n_seq, blk, dm = x_in.shape
    seq = 4 * blk
    qw = wq.shape[1] // 2
    hd = wkv.shape[1] // 4
    n_heads = qw // hd
    kw = qw + 2 * hd
    any_spec = pl.BlockSpec(memory_space=pl.ANY)
    dma = pltpu.SemaphoreType.DMA
    rows = n_seq * seq
    flops = 2 * rows * dm * (2 * kw + 2 * qw) + 12 * n_seq * n_heads * seq * seq * hd
    return pl.pallas_call(
        group_kernel,
        out_shape=(
            jax.ShapeDtypeStruct((4, n_seq, blk, dm), BF16),
            jax.ShapeDtypeStruct((4, n_seq, blk, dm), BF16),
            jax.ShapeDtypeStruct((qw, dm), F32),
            jax.ShapeDtypeStruct((kw, dm), F32),
            jax.ShapeDtypeStruct((n_seq, blk, 2 * qw), BF16),
            jax.ShapeDtypeStruct((n_seq, blk, 2 * kw), BF16),
            jax.ShapeDtypeStruct((n_seq, blk, dm), BF16),
        ),
        in_specs=[any_spec] * 6,
        out_specs=(any_spec,) * 7,
        scratch_shapes=[
            pltpu.VMEM((2, seq, dm), BF16), pltpu.VMEM((2, seq, dm), BF16), pltpu.VMEM((1, dm), F32),
            pltpu.VMEM((dm, kw), BF16), pltpu.VMEM((qw, dm), BF16),
            pltpu.VMEM((qw, dm), F32), pltpu.VMEM((kw, dm), F32),
            pltpu.VMEM((n_heads, seq, hd), BF16), pltpu.VMEM((n_heads, seq, hd), BF16),
            pltpu.VMEM((seq, hd), BF16), pltpu.VMEM((seq, hd), BF16),
            pltpu.VMEM((hd, seq), BF16), pltpu.VMEM((hd, seq), BF16),
            pltpu.VMEM((qw, seq), BF16), pltpu.VMEM((kw, seq), BF16),
            pltpu.VMEM((seq, hd), F32), pltpu.VMEM((seq, hd), F32),
            pltpu.VMEM((2 * blk, qw), BF16), pltpu.VMEM((2 * blk, kw), BF16),
            dma((2, n_seq)), dma((2, n_seq)), dma((2, n_seq)), dma((2, n_seq)), dma((2, n_seq)), dma((2, n_seq)),
            dma((2, 4)), dma((4,)), dma((2,)), dma((2,)), dma((2, n_seq)), dma((2,)), dma((2, 2)),
        ],
        cost_estimate=pl.CostEstimate(flops=flops, bytes_accessed=400_000_000, transcendentals=0),
        compiler_params=pltpu.CompilerParams(collective_id=0, has_side_effects=True, vmem_limit_bytes=67_000_000),
    )(x_in, dy_in, gain, wq, wkv, wo)


def dx_kernel(dq, w_all, x, dy, gain, dx, dg, dn):
    i = pl.program_id(0)
    n_tiles = pl.num_programs(0) - 1
    tm, dm = x.shape
    parts = 4
    cw = dm // parts
    cr = tm // parts

    def matmul(n):
        cols = pl.ds(pl.multiple_of(n * cw, cw), cw)
        dn[i % 2, :, cols] = dot_nt(dq[...], w_all[cols, :])

    def finish(n):
        rows = pl.ds(pl.multiple_of(n * cr, 16), cr)
        xf = x[rows, :].astype(F32)
        r = lax.rsqrt(jnp.mean(xf * xf, axis=-1, keepdims=True) + EPS)
        u = xf * r
        d = dn[(i + 1) % 2, rows, :]
        du = d * u
        dg[...] += jnp.sum(du.reshape(cr // 8, 8, dm), axis=0)
        g = gain[...]
        mean_eu = jnp.mean(du * g, axis=-1, keepdims=True)
        dx[rows, :] = (dy[rows, :].astype(F32) + r * (d * g - u * mean_eu)).astype(BF16)

    @pl.when(i == 0)
    def _():
        dg[...] = jnp.zeros_like(dg)

        @pl.loop(0, parts)
        def _(n):
            matmul(n)

    @pl.when(jnp.logical_and(i > 0, i < n_tiles))
    def _():
        @pl.loop(0, parts)
        def _(n):
            finish(n)
            matmul(n)

    @pl.when(i == n_tiles)
    def _():
        @pl.loop(0, parts)
        def _(n):
            finish(n)


def dx_call(dq, w_all, x, dy, gain):
    rows, dm = x.shape
    kw = dq.shape[1]
    tm = 384
    n_tiles = rows // tm
    late = lambda i: (jnp.maximum(i - 1, 0), 0)
    return pl.pallas_call(
        dx_kernel,
        grid=(n_tiles + 1,),
        out_shape=(jax.ShapeDtypeStruct((rows, dm), BF16), jax.ShapeDtypeStruct((8, dm), F32)),
        in_specs=[pl.BlockSpec((tm, kw), lambda i: (jnp.minimum(i, n_tiles - 1), 0)),
                  pl.BlockSpec((dm, kw), lambda i: (0, 0)),
                  pl.BlockSpec((tm, dm), late), pl.BlockSpec((tm, dm), late),
                  pl.BlockSpec((1, dm), lambda i: (0, 0))],
        out_specs=(pl.BlockSpec((tm, dm), late), pl.BlockSpec((8, dm), lambda i: (0, 0))),
        scratch_shapes=[pltpu.VMEM((2, tm, dm), F32)],
        cost_estimate=pl.CostEstimate(flops=2 * rows * dm * kw, bytes_accessed=50_000_000, transcendentals=0),
        compiler_params=pltpu.CompilerParams(vmem_limit_bytes=60_000_000),
    )(dq, w_all, x, dy, gain)


def y_kernel(core_ref, o, wo, x, own_o, recv_o, own_q, recv_q, y, d_wo, d_wq, d_wk, d_wv):
    i = pl.program_id(0)
    core = core_ref[0]
    n_heads, hd = d_wq.shape[1], d_wq.shape[2]
    n_group = n_heads // 2
    y[...] = (x[...].astype(F32) + dot_nn(o[...], wo[...])).astype(BF16)
    mine = i // (pl.num_programs(0) // 2) == core
    d_wo[...] = jnp.where(mine, own_o[...], recv_o[...])
    for g in range(2):
        own = core == g
        for h in range(n_group + 2):
            rows = pl.ds(h * hd, hd)
            val = jnp.where(own, own_q[rows, :], recv_q[rows, :]).T
            if h < n_group:
                d_wq[:, g * n_group + h, :] = val
            elif h == n_group:
                d_wk[:, g, :] = val
            else:
                d_wv[:, g, :] = val


def y_call(core, o, wo, x, own_o, recv_o, own_q, recv_q, n_heads, hd):
    rows, dm = x.shape
    qw2 = o.shape[1]
    kw = own_q.shape[0]
    steps = 8
    tm = rows // steps
    tw = qw2 // steps
    tn = dm // steps
    hs = steps // 2
    grid_spec = pltpu.PrefetchScalarGridSpec(
        num_scalar_prefetch=1,
        grid=(steps,),
        in_specs=[pl.BlockSpec((tm, qw2), lambda i, c: (i, 0)),
                  pl.BlockSpec((qw2, dm), lambda i, c: (0, 0)),
                  pl.BlockSpec((tm, dm), lambda i, c: (i, 0)),
                  pl.BlockSpec((tw, dm), lambda i, c: (jnp.clip(i - hs * c[0], 0, hs - 1), 0)),
                  pl.BlockSpec((tw, dm), lambda i, c: (jnp.clip(i - hs * (1 - c[0]), 0, hs - 1), 0)),
                  pl.BlockSpec((kw, tn), lambda i, c: (0, i)),
                  pl.BlockSpec((kw, tn), lambda i, c: (0, i))],
        out_specs=(pl.BlockSpec((tm, dm), lambda i, c: (i, 0)),
                   pl.BlockSpec((tw, dm), lambda i, c: (i, 0)),
                   pl.BlockSpec((tn, n_heads, hd), lambda i, c: (i, 0, 0)),
                   pl.BlockSpec((tn, 2, hd), lambda i, c: (i, 0, 0)),
                   pl.BlockSpec((tn, 2, hd), lambda i, c: (i, 0, 0))))
    return pl.pallas_call(
        y_kernel,
        grid_spec=grid_spec,
        out_shape=(jax.ShapeDtypeStruct((rows, dm), BF16), jax.ShapeDtypeStruct((qw2, dm), F32),
                   jax.ShapeDtypeStruct((dm, n_heads, hd), F32),
                   jax.ShapeDtypeStruct((dm, 2, hd), F32), jax.ShapeDtypeStruct((dm, 2, hd), F32)),
        cost_estimate=pl.CostEstimate(flops=2 * rows * dm * qw2, bytes_accessed=110_000_000, transcendentals=0),
        compiler_params=pltpu.CompilerParams(vmem_limit_bytes=60_000_000),
    )(core, o, wo, x, own_o, recv_o, own_q, recv_q)


def solution(mesh):
    def device_fn(x_in, dy_in, norm_gain, w_q, w_k, w_v, w_o):
        n_batch, blk, dm = x_in.shape
        n_heads, hd = w_q.shape[1], w_q.shape[2]
        rows = n_batch * blk
        qw = n_heads * hd // 2
        core = (lax.axis_index('cp') % 2).astype(jnp.int32).reshape(1)
        gain = norm_gain.astype(F32).reshape(1, dm)
        wq = w_q.reshape(dm, n_heads * hd)
        wkv = jnp.concatenate([w_k, w_v], axis=2).reshape(dm, 4 * hd)
        wo = w_o.reshape(n_heads * hd, dm)

        _, _, dwo_own, dwq_own, o_own, dq_own, _ = group_call(x_in, dy_in, gain, wq, wkv, wo)

        n_dev = mesh.shape['cp']
        pair_perm = [(d, d ^ 1) for d in range(n_dev)]
        dwo_recv, dwq_recv = lax.ppermute((dwo_own, dwq_own), 'cp', pair_perm)

        w_all = jnp.concatenate([wq[:, :qw], wkv[:, :2 * hd], wq[:, qw:], wkv[:, 2 * hd:]], axis=1)
        x2 = x_in.reshape(rows, dm)
        dx, dg = dx_call(dq_own.reshape(rows, -1), w_all, x2, dy_in.reshape(rows, dm), gain)
        dg = jnp.sum(dg, axis=0)
        dg1 = lax.ppermute(dg, 'cp', pair_perm)
        dg2 = lax.ppermute(dg, 'cp', [(d, d ^ 2) for d in range(n_dev)])
        dg3 = lax.ppermute(dg, 'cp', [(d, d ^ 3) for d in range(n_dev)])
        d_gain = (dg + dg1) + (dg2 + dg3)
        y, d_wo, d_wq, d_wk, d_wv = y_call(core, o_own.reshape(rows, -1), wo, x2, dwo_own, dwo_recv, dwq_own, dwq_recv,
                                           n_heads, hd)
        return (y.reshape(x_in.shape), dx.reshape(x_in.shape), d_gain, d_wq, d_wk, d_wv, d_wo.reshape(n_heads, hd, dm))

    act_spec = P('dp', 'cp', None)
    mat_spec = P(None, None, None)
    grad_spec = P('dp', None, None)
    return jax.shard_map(device_fn, mesh=mesh,
                         in_specs=(act_spec, act_spec, P(None), mat_spec, mat_spec, mat_spec, mat_spec),
                         out_specs=(act_spec, act_spec, P('dp'), grad_spec, grad_spec, grad_spec, grad_spec),
                         check_vma=False)
```

```python
import functools

import jax
import jax.numpy as jnp
from jax import lax
from jax.experimental import pallas as pl
from jax.experimental.pallas import tpu as pltpu
from jax.sharding import PartitionSpec as P

EPS = 1e-6
F32 = jnp.float32
BF16 = jnp.bfloat16
LOG2E = 1.4426950408889634
MESH = pl.DeviceIdType.MESH
CROSS_AHEAD = 4
PAIR_AHEAD = 2


def dot_nn(a, b):
    return lax.dot_general(a, b, (((1,), (0,)), ((), ())), preferred_element_type=F32)


def dot_nt(a, b):
    return lax.dot_general(a, b, (((1,), (1,)), ((), ())), preferred_element_type=F32)


def group_kernel(x, dy, gain, w_q, wkv, wo, gx, gy, dwo, dwq, oo, dqo, xn, wq,
                 xb, yb, gain_v, w_in, w_f32, wq_v, wo_v, acc_o, acc_q, q_s, do_s, k_s, v_s, kt_s, vt_s,
                 ot_s, dqt_s, dk_acc, dv_acc, o_n, dq_n,
                 cs, cr, ds, dr, fs, fr, lsem, wsem, osem, psend, precv, fsem, nsem, rsem):
    n_seq, blk, dm = x.shape
    seq = 4 * blk
    n_heads, _, hd = q_s.shape
    qw = n_heads * hd
    half = 2 * blk
    tile = 256
    n_tiles = seq // tile
    c2 = LOG2E * hd ** -0.5
    scale = hd ** -0.5

    me = lax.axis_index('cp')
    core = me % 2
    chip = me // 2
    pair = chip * 2 + (1 - core)
    across = (1 - chip) * 2 + core
    diag = (1 - chip) * 2 + (1 - core)
    src_of = (xn, dy)
    land_of = (gx, gy)
    vmem_of = (xb, yb)

    def cross_copy(t, s):
        return pltpu.make_async_remote_copy(src_of[t].at[s], land_of[t].at[me, s], cs.at[t, s], cr.at[t, s],
                                            device_id={'cp': across}, device_id_type=MESH)

    def cross_arrival(t, s):
        return pltpu.make_async_remote_copy(src_of[t].at[s], land_of[t].at[across, s], cs.at[t, s], cr.at[t, s],
                                            device_id={'cp': across}, device_id_type=MESH)

    def pair_copy(t, s):
        return pltpu.make_async_remote_copy(src_of[t].at[s], land_of[t].at[me, s], ds.at[t, s], dr.at[t, s],
                                            device_id={'cp': pair}, device_id_type=MESH)

    def pair_arrival(t, s):
        return pltpu.make_async_remote_copy(src_of[t].at[s], land_of[t].at[pair, s], ds.at[t, s], dr.at[t, s],
                                            device_id={'cp': pair}, device_id_type=MESH)

    def fwd_copy(t, s):
        return pltpu.make_async_remote_copy(land_of[t].at[across, s], land_of[t].at[across, s], fs.at[t, s], fr.at[t, s],
                                            device_id={'cp': pair}, device_id_type=MESH)

    def fwd_arrival(t, s):
        return pltpu.make_async_remote_copy(land_of[t].at[across, s], land_of[t].at[diag, s], fs.at[t, s], fr.at[t, s],
                                            device_id={'cp': pair}, device_id_type=MESH)

    def rows_of(b):
        return pl.ds(pl.multiple_of(b * blk, 64), blk)

    def load_own(t, s):
        return pltpu.make_async_copy(src_of[t].at[s], vmem_of[t].at[s % 2, rows_of(me)], lsem.at[t, 0])

    def load_from(t, s, b, j):
        return pltpu.make_async_copy(land_of[t].at[b, s], vmem_of[t].at[s % 2, rows_of(b)], lsem.at[t, j])

    kvw = 2 * hd

    def out_parts(s, g):
        q_cols = pl.ds(pl.multiple_of(g * qw, 128), qw)
        kv_cols = pl.ds(pl.multiple_of(2 * qw + g * kvw, 128), kvw)
        return ((o_n, slice(0, qw), oo.at[s, :, q_cols]),
                (dq_n, slice(0, qw), dqo.at[s, :, q_cols]),
                (dq_n, slice(qw, qw + kvw), dqo.at[s, :, kv_cols]))

    def pair_send(idx, s, buf, cols, dst):
        rows = pl.ds(pl.multiple_of((1 - core) * blk, 64), blk)
        return pltpu.make_async_remote_copy(buf.at[rows, cols], dst, psend.at[idx], precv.at[idx, s],
                                            device_id={'cp': pair}, device_id_type=MESH)

    def out_copies(s):
        rows = pl.ds(pl.multiple_of(core * blk, 64), blk)
        return [(pltpu.make_async_copy(buf.at[rows, cols], dst, osem.at[idx]), pair_send(idx, s, buf, cols, dst))
                for idx, (buf, cols, dst) in enumerate(out_parts(s, core))]

    def out_arrivals(s):
        return [pair_send(idx, s, buf, cols, dst) for idx, (buf, cols, dst) in enumerate(out_parts(s, 1 - core))]

    weight_loads = [
        pltpu.make_async_copy(gain, gain_v, wsem.at[0]),
        pltpu.make_async_copy(wq.at[:, pl.ds(pl.multiple_of(core * qw, 128), qw)], wq_v.at[:, 0:qw], wsem.at[1]),
        pltpu.make_async_copy(wkv.at[:, pl.ds(pl.multiple_of(core * kvw, 128), kvw)], wq_v.at[:, qw:qw + kvw], wsem.at[2]),
        pltpu.make_async_copy(wo.at[pl.ds(pl.multiple_of(core * qw, 128), qw)], wo_v, wsem.at[3]),
    ]

    def norm_in(s):
        return pltpu.make_async_copy(x.at[s], yb.at[1, pl.ds(pl.multiple_of((s % 2) * blk, 64), blk)], nsem.at[0, s % 2])

    def norm_out(s):
        return pltpu.make_async_copy(xb.at[1, pl.ds(pl.multiple_of((s % 2) * blk, 64), blk)], xn.at[s], nsem.at[1, s % 2])

    n_wrows = w_in.shape[1]
    n_wsteps = dm // n_wrows
    stage0 = half

    def relay_in(c):
        return pltpu.make_async_copy(w_q.at[pl.ds(pl.multiple_of(c * n_wrows, n_wrows), n_wrows)], w_in.at[c % 2],
                                     rsem.at[0, c % 2])

    def relay_out(c):
        return pltpu.make_async_copy(xb.at[1, pl.ds(pl.multiple_of(stage0 + (c % 2) * n_wrows, n_wrows), n_wrows)],
                                     wq.at[pl.ds(pl.multiple_of(c * n_wrows, n_wrows), n_wrows)], rsem.at[1, c % 2])

    def relay_step(c, carry):
        @pl.when(c + 1 < n_wsteps)
        def _():
            relay_in(c + 1).start()
        relay_in(c).wait()

        @pl.when(c > 1)
        def _():
            relay_out(c - 2).wait()
        w_f32[...] = w_in[c % 2].astype(F32)
        rows = pl.ds(pl.multiple_of(stage0 + (c % 2) * n_wrows, n_wrows), n_wrows)
        for h in range(2 * n_heads):
            xb[1, rows, h * hd:(h + 1) * hd] = w_f32[:, h, :].astype(BF16)
        relay_out(c).start()
        return carry

    norm_in(0).start()
    relay_in(0).start()
    for copy in (weight_loads[0], weight_loads[2], weight_loads[3]):
        copy.start()

    barrier = pltpu.get_barrier_semaphore()
    for peer in (pair, across):
        pl.semaphore_signal(barrier, inc=1, device_id={'cp': peer}, device_id_type=MESH)
    pl.semaphore_wait(barrier, 2)

    cross_copy(1, 0).start()
    pair_copy(1, 0).start()
    load_own(1, 0).start()
    weight_loads[0].wait()

    def send_normed(s):
        norm_out(s).wait()

        @pl.when(s < CROSS_AHEAD)
        def _():
            cross_copy(0, s).start()

        @pl.when(s + 1 < CROSS_AHEAD)
        def _():
            cross_copy(1, s + 1).start()

        @pl.when(s < PAIR_AHEAD)
        def _():
            pair_copy(0, s).start()

        @pl.when(s + 1 < PAIR_AHEAD)
        def _():
            pair_copy(1, s + 1).start()

    def norm_step(s, carry):
        @pl.when(s + 1 < n_seq)
        def _():
            norm_in(s + 1).start()
        norm_in(s).wait()
        base = (s % 2) * blk
        for c in range(blk // 48):
            rows = pl.ds(pl.multiple_of(base + c * 48, 16), 48)
            xf = yb[1, rows, :].astype(F32)
            r = lax.rsqrt(jnp.mean(xf * xf, axis=-1, keepdims=True) + EPS)
            xb[1, rows, :] = (xf * r * gain_v[...]).astype(BF16)
        norm_out(s).start()

        @pl.when(s > 0)
        def _():
            send_normed(s - 1)
        return carry

    lax.fori_loop(0, n_seq, norm_step, 0)
    send_normed(n_seq - 1)
    load_own(0, 0).start()
    lax.fori_loop(0, n_wsteps, relay_step, 0)
    relay_out(n_wsteps - 2).wait()
    relay_out(n_wsteps - 1).wait()
    weight_loads[1].start()
    acc_o[...] = jnp.zeros_like(acc_o)
    acc_q[...] = jnp.zeros_like(acc_q)
    for t in range(2):
        pair_arrival(t, 0).wait_recv()
        load_from(t, 0, pair, 1).start()
    for copy in weight_loads[1:]:
        copy.wait()

    def project_x(slot, r0):
        rows = pl.ds(pl.multiple_of(r0, 128), half)
        for n in range((qw + 2 * hd) // tile):
            res = dot_nn(xb[slot, rows, :], wq_v[:, n * tile:(n + 1) * tile]).astype(BF16)
            for part in range(tile // hd):
                col = n * tile + part * hd
                piece = res[:, part * hd:(part + 1) * hd]
                if col < qw:
                    q_s[col // hd, rows, :] = piece
                elif col == qw:
                    k_s[rows, :] = piece
                else:
                    v_s[rows, :] = piece

    def project_dy(slot, r0):
        rows = pl.ds(pl.multiple_of(r0, 128), half)
        for n in range(qw // tile):
            res = dot_nt(yb[slot, rows, :], wo_v[n * tile:(n + 1) * tile, :]).astype(BF16)
            for part in range(tile // hd):
                do_s[(n * tile + part * hd) // hd, rows, :] = res[:, part * hd:(part + 1) * hd]

    def heads():
        units = [(h, i) for h in range(n_heads) for i in range(n_tiles)]
        state = {}

        def score(u):
            h, i = units[u]
            nk = (i + 1) * tile
            qi = q_s[h, i * tile:(i + 1) * tile, :]
            doi = do_s[h, i * tile:(i + 1) * tile, :]
            state[u] = [dot_nt(k_s[0:nk, :], qi), dot_nt(v_s[0:nk, :], doi)]

        def attend(u):
            h, i = units[u]
            nk = (i + 1) * tile
            st, dpt = state[u]
            key_pos = lax.broadcasted_iota(jnp.int32, (tile, tile), 0)
            qry_pos = lax.broadcasted_iota(jnp.int32, (tile, tile), 1)
            edge = jnp.where(key_pos <= qry_pos, st[nk - tile:], -jnp.inf)
            st = edge if i == 0 else jnp.concatenate([st[:nk - tile], edge], axis=0)
            mx = jnp.max(st, axis=0, keepdims=True)
            p = jnp.exp2(st * c2 - mx * c2)
            inv_l = 1.0 / jnp.sum(p, axis=0, keepdims=True)
            ot = (dot_nn(vt_s[:, 0:nk], p.astype(BF16)) * inv_l).astype(BF16)
            ot_s[h * hd:(h + 1) * hd, i * tile:(i + 1) * tile] = ot
            state[u] = [p, inv_l, ot, dpt]

        def grads(u):
            h, i = units[u]
            nk = (i + 1) * tile
            p, inv_l, ot, dpt = state.pop(u)
            qi = q_s[h, i * tile:(i + 1) * tile, :]
            doi = do_s[h, i * tile:(i + 1) * tile, :]
            delta = jnp.sum(doi.astype(F32).T * ot.astype(F32), axis=0, keepdims=True)
            pn = p * inv_l
            dst = (pn * (dpt - delta) * scale).astype(BF16)
            dv_acc[0:nk, :] += dot_nn(pn.astype(BF16), doi)
            dk_acc[0:nk, :] += dot_nn(dst, qi)
            dqt_s[h * hd:(h + 1) * hd, i * tile:(i + 1) * tile] = dot_nn(kt_s[:, 0:nk], dst).astype(BF16)

        for t in range(-2, len(units)):
            if t + 2 < len(units):
                score(t + 2)
            if 0 <= t + 1 < len(units):
                attend(t + 1)
            if t >= 0:
                grads(t)
        own_cols = pl.ds(pl.multiple_of(chip * half, 128), half)
        for h in range(n_heads):
            o_n[:, h * hd:(h + 1) * hd] = ot_s[h * hd:(h + 1) * hd, own_cols].T
            dq_n[:, h * hd:(h + 1) * hd] = dqt_s[h * hd:(h + 1) * hd, own_cols].T

    def seq_step(s, carry):
        slot = s % 2
        @pl.when(s + CROSS_AHEAD < n_seq)
        def _():
            for t in range(2):
                cross_copy(t, s + CROSS_AHEAD).start()
        @pl.when(s + PAIR_AHEAD < n_seq)
        def _():
            for t in range(2):
                pair_copy(t, s + PAIR_AHEAD).start()

        cross_arrival(0, s).wait_recv()
        fwd_copy(0, s).start()
        load_from(0, s, across, 2).start()
        for t in range(2):
            load_own(t, s).wait()
            load_from(t, s, pair, 1).wait()
        near = chip * half
        far = (1 - chip) * half
        project_x(slot, near)
        project_dy(slot, near)
        fwd_arrival(0, s).wait_recv()
        load_from(0, s, diag, 3).start()
        load_from(0, s, across, 2).wait()
        load_from(0, s, diag, 3).wait()
        project_x(slot, far)
        cross_arrival(1, s).wait_recv()
        fwd_copy(1, s).start()
        load_from(1, s, across, 2).start()
        fwd_arrival(1, s).wait_recv()
        load_from(1, s, diag, 3).start()

        kt_s[...] = k_s[...].T
        vt_s[...] = v_s[...].T
        dk_acc[...] = jnp.zeros_like(dk_acc)
        dv_acc[...] = jnp.zeros_like(dv_acc)
        load_from(1, s, across, 2).wait()
        load_from(1, s, diag, 3).wait()
        project_dy(slot, far)

        @pl.when(s + 1 < n_seq)
        def _():
            for t in range(2):
                load_own(t, s + 1).start()
                pair_arrival(t, s + 1).wait_recv()
                load_from(t, s + 1, pair, 1).start()

        @pl.when(s > 0)
        def _():
            for local, remote in out_copies(s - 1):
                local.wait()
                remote.wait_send()

        heads()

        near_rows = pl.ds(pl.multiple_of(near, 128), half)
        for idx, acc in enumerate((dk_acc, dv_acc)):
            lo = qw + idx * hd
            dqt_s[lo:lo + hd, :] = acc[...].T.astype(BF16)
            dq_n[:, lo:lo + hd] = acc[near_rows, :].astype(BF16)
        for local, remote in out_copies(s):
            local.start()
            remote.start()

        def dwo_step(n, c):
            cols = pl.ds(pl.multiple_of(n * 2 * tile, 2 * tile), 2 * tile)
            acc_o[:, cols] += dot_nn(ot_s[...], yb[slot, :, cols])
            return c

        lax.fori_loop(0, dm // (2 * tile), dwo_step, 0)

        @pl.when(s == n_seq - 1)
        def _():
            flush_o.start()

        def dwq_step(n, c):
            cols = pl.ds(pl.multiple_of(n * 2 * tile, 2 * tile), 2 * tile)
            acc_q[:, cols] += dot_nn(dqt_s[...], xb[slot, :, cols])

            @pl.when(s == n_seq - 1)
            def _():
                flush_q(n).start()
            return c

        lax.fori_loop(0, dm // (2 * tile), dwq_step, 0)
        return carry

    flush_o = pltpu.make_async_copy(acc_o, dwo, fsem.at[0])

    def flush_q(n):
        cols = pl.ds(pl.multiple_of(n * 2 * tile, 2 * tile), 2 * tile)
        return pltpu.make_async_copy(acc_q.at[:, cols], dwq.at[:, cols], fsem.at[1 + n])

    lax.fori_loop(0, n_seq, seq_step, 0)

    for local, remote in out_copies(n_seq - 1):
        local.wait()
        remote.wait_send()

    def drain(s, carry):
        for t in range(2):
            cross_copy(t, s).wait_send()
            pair_copy(t, s).wait_send()
            fwd_copy(t, s).wait_send()
        for arrival in out_arrivals(s):
            arrival.wait_recv()
        return carry

    lax.fori_loop(0, n_seq, drain, 0)
    flush_o.wait()
    for n in range(dm // (2 * tile)):
        flush_q(n).wait()


def group_call(x_in, dy_in, gain, w_q, wkv, wo):
    n_seq, blk, dm = x_in.shape
    seq = 4 * blk
    n_heads, hd = w_q.shape[1] // 2, w_q.shape[2]
    qw = n_heads * hd
    kw = qw + 2 * hd
    any_spec = pl.BlockSpec(memory_space=pl.ANY)
    dma = pltpu.SemaphoreType.DMA
    rows = n_seq * seq
    flops = 2 * rows * dm * (2 * kw + 2 * qw) + 12 * n_seq * n_heads * seq * seq * hd
    return pl.pallas_call(
        group_kernel,
        out_shape=(
            jax.ShapeDtypeStruct((4, n_seq, blk, dm), BF16),
            jax.ShapeDtypeStruct((4, n_seq, blk, dm), BF16),
            jax.ShapeDtypeStruct((qw, dm), F32),
            jax.ShapeDtypeStruct((kw, dm), F32),
            jax.ShapeDtypeStruct((n_seq, blk, 2 * qw), BF16),
            jax.ShapeDtypeStruct((n_seq, blk, 2 * kw), BF16),
            jax.ShapeDtypeStruct((n_seq, blk, dm), BF16),
            jax.ShapeDtypeStruct((dm, 2 * qw), BF16),
        ),
        in_specs=[any_spec] * 6,
        out_specs=(any_spec,) * 8,
        scratch_shapes=[
            pltpu.VMEM((2, seq, dm), BF16), pltpu.VMEM((2, seq, dm), BF16), pltpu.VMEM((1, dm), F32),
            pltpu.VMEM((2, 64, 2 * n_heads, hd), BF16), pltpu.VMEM((64, 2 * n_heads, hd), F32),
            pltpu.VMEM((dm, kw), BF16), pltpu.VMEM((qw, dm), BF16),
            pltpu.VMEM((qw, dm), F32), pltpu.VMEM((kw, dm), F32),
            pltpu.VMEM((n_heads, seq, hd), BF16), pltpu.VMEM((n_heads, seq, hd), BF16),
            pltpu.VMEM((seq, hd), BF16), pltpu.VMEM((seq, hd), BF16),
            pltpu.VMEM((hd, seq), BF16), pltpu.VMEM((hd, seq), BF16),
            pltpu.VMEM((qw, seq), BF16), pltpu.VMEM((kw, seq), BF16),
            pltpu.VMEM((seq, hd), F32), pltpu.VMEM((seq, hd), F32),
            pltpu.VMEM((2 * blk, qw), BF16), pltpu.VMEM((2 * blk, kw), BF16),
            dma((2, n_seq)), dma((2, n_seq)), dma((2, n_seq)), dma((2, n_seq)), dma((2, n_seq)), dma((2, n_seq)),
            dma((2, 4)), dma((4,)), dma((3,)), dma((3,)), dma((3, n_seq)), dma((1 + dm // 512,)), dma((2, 2)), dma((2, 2)),
        ],
        cost_estimate=pl.CostEstimate(flops=flops, bytes_accessed=400_000_000, transcendentals=0),
        compiler_params=pltpu.CompilerParams(collective_id=0, has_side_effects=True, vmem_limit_bytes=67_000_000),
    )(x_in, dy_in, gain, w_q, wkv, wo)


def dx_kernel(dq, wq, wkv, x, dy, gain, dx, dg, dn, w_all, wsem):
    i = pl.program_id(0)
    n_tiles = pl.num_programs(0) - 1
    tm, dm = x.shape
    parts = 4
    cw = dm // parts
    cr = tm // parts

    def matmul(n):
        cols = pl.ds(pl.multiple_of(n * cw, cw), cw)
        dn[i % 2, :, cols] = dot_nt(dq[...], w_all[cols, :])

    def finish(n):
        rows = pl.ds(pl.multiple_of(n * cr, 16), cr)
        xf = x[rows, :].astype(F32)
        r = lax.rsqrt(jnp.mean(xf * xf, axis=-1, keepdims=True) + EPS)
        u = xf * r
        d = dn[(i + 1) % 2, rows, :]
        du = d * u
        dg[...] += jnp.sum(du.reshape(cr // 8, 8, dm), axis=0)
        g = gain[...]
        mean_eu = jnp.mean(du * g, axis=-1, keepdims=True)
        dx[rows, :] = (dy[rows, :].astype(F32) + r * (d * g - u * mean_eu)).astype(BF16)

    @pl.when(i == 0)
    def _():
        qw = wq.shape[1]

        def loads(n):
            rows = pl.ds(pl.multiple_of(n * cw, cw), cw)
            return (pltpu.make_async_copy(wq.at[rows], w_all.at[rows, 0:qw], wsem.at[0, n]),
                    pltpu.make_async_copy(wkv.at[rows], w_all.at[rows, qw:], wsem.at[1, n]))

        for n in range(parts):
            for copy in loads(n):
                copy.start()
        dg[...] = jnp.zeros_like(dg)

        @pl.loop(0, parts)
        def _(n):
            for copy in loads(n):
                copy.wait()
            matmul(n)

    @pl.when(jnp.logical_and(i > 0, i < n_tiles))
    def _():
        @pl.loop(0, parts)
        def _(n):
            finish(n)
            matmul(n)

    @pl.when(i == n_tiles)
    def _():
        @pl.loop(0, parts)
        def _(n):
            finish(n)


def dx_call(dq, wq, wkv, x, dy, gain):
    rows, dm = x.shape
    kw = dq.shape[1]
    tm = 384
    n_tiles = rows // tm
    late = lambda i: (jnp.maximum(i - 1, 0), 0)
    any_spec = pl.BlockSpec(memory_space=pl.ANY)
    return pl.pallas_call(
        dx_kernel,
        grid=(n_tiles + 1,),
        out_shape=(jax.ShapeDtypeStruct((rows, dm), BF16), jax.ShapeDtypeStruct((8, dm), F32)),
        in_specs=[pl.BlockSpec((tm, kw), lambda i: (jnp.minimum(i, n_tiles - 1), 0)),
                  any_spec, any_spec,
                  pl.BlockSpec((tm, dm), late), pl.BlockSpec((tm, dm), late),
                  pl.BlockSpec((1, dm), lambda i: (0, 0))],
        out_specs=(pl.BlockSpec((tm, dm), late), pl.BlockSpec((8, dm), lambda i: (0, 0))),
        scratch_shapes=[pltpu.VMEM((2, tm, dm), F32), pltpu.VMEM((dm, kw), BF16), pltpu.SemaphoreType.DMA((2, 4))],
        cost_estimate=pl.CostEstimate(flops=2 * rows * dm * kw, bytes_accessed=50_000_000, transcendentals=0),
        compiler_params=pltpu.CompilerParams(vmem_limit_bytes=60_000_000),
    )(dq, wq, wkv, x, dy, gain)


def y_kernel(core_ref, o, wo, x, own_o, recv_o, own_q, recv_q, y, d_wo, d_wq, d_wk, d_wv, wo_v, wsem):
    i = pl.program_id(0)
    core = core_ref[0]
    n_heads, hd = d_wq.shape[1], d_wq.shape[2]
    n_group = n_heads // 2
    load = pltpu.make_async_copy(wo, wo_v, wsem)

    def place():
        mine = i // (pl.num_programs(0) // 2) == core
        d_wo[...] = jnp.where(mine, own_o[...], recv_o[...])
        for g in range(2):
            own = core == g
            for h in range(n_group + 2):
                rows = pl.ds(h * hd, hd)
                val = jnp.where(own, own_q[rows, :], recv_q[rows, :]).T
                if h < n_group:
                    d_wq[:, g * n_group + h, :] = val
                elif h == n_group:
                    d_wk[:, g, :] = val
                else:
                    d_wv[:, g, :] = val

    def project():
        y[...] = (x[...].astype(F32) + dot_nn(o[...], wo_v[...])).astype(BF16)

    @pl.when(i == 0)
    def _():
        load.start()
        place()
        load.wait()
        project()

    @pl.when(i > 0)
    def _():
        project()
        place()


def y_call(core, o, wo, x, own_o, recv_o, own_q, recv_q, n_heads, hd):
    rows, dm = x.shape
    qw2 = o.shape[1]
    kw = own_q.shape[0]
    steps = 8
    tm = rows // steps
    tw = qw2 // steps
    tn = dm // steps
    hs = steps // 2
    grid_spec = pltpu.PrefetchScalarGridSpec(
        num_scalar_prefetch=1,
        grid=(steps,),
        in_specs=[pl.BlockSpec((tm, qw2), lambda i, c: (i, 0)),
                  pl.BlockSpec(memory_space=pl.ANY),
                  pl.BlockSpec((tm, dm), lambda i, c: (i, 0)),
                  pl.BlockSpec((tw, dm), lambda i, c: (jnp.clip(i - hs * c[0], 0, hs - 1), 0)),
                  pl.BlockSpec((tw, dm), lambda i, c: (jnp.clip(i - hs * (1 - c[0]), 0, hs - 1), 0)),
                  pl.BlockSpec((kw, tn), lambda i, c: (0, i)),
                  pl.BlockSpec((kw, tn), lambda i, c: (0, i))],
        out_specs=(pl.BlockSpec((tm, dm), lambda i, c: (i, 0)),
                   pl.BlockSpec((tw, dm), lambda i, c: (i, 0)),
                   pl.BlockSpec((tn, n_heads, hd), lambda i, c: (i, 0, 0)),
                   pl.BlockSpec((tn, 2, hd), lambda i, c: (i, 0, 0)),
                   pl.BlockSpec((tn, 2, hd), lambda i, c: (i, 0, 0))),
        scratch_shapes=[pltpu.VMEM((qw2, dm), BF16), pltpu.SemaphoreType.DMA])
    return pl.pallas_call(
        y_kernel,
        grid_spec=grid_spec,
        out_shape=(jax.ShapeDtypeStruct((rows, dm), BF16), jax.ShapeDtypeStruct((qw2, dm), F32),
                   jax.ShapeDtypeStruct((dm, n_heads, hd), F32),
                   jax.ShapeDtypeStruct((dm, 2, hd), F32), jax.ShapeDtypeStruct((dm, 2, hd), F32)),
        cost_estimate=pl.CostEstimate(flops=2 * rows * dm * qw2, bytes_accessed=110_000_000, transcendentals=0),
        compiler_params=pltpu.CompilerParams(vmem_limit_bytes=60_000_000),
    )(core, o, wo, x, own_o, recv_o, own_q, recv_q)


def solution(mesh):
    def device_fn(x_in, dy_in, norm_gain, w_q, w_k, w_v, w_o):
        n_batch, blk, dm = x_in.shape
        n_heads, hd = w_q.shape[1], w_q.shape[2]
        rows = n_batch * blk
        qw = n_heads * hd // 2
        core = (lax.axis_index('cp') % 2).astype(jnp.int32).reshape(1)
        gain = norm_gain.astype(F32).reshape(1, dm)
        wkv = jnp.concatenate([w_k, w_v], axis=2).reshape(dm, 4 * hd)
        wo = w_o.reshape(n_heads * hd, dm)

        _, _, dwo_own, dwq_own, o_own, dq_own, _, wq = group_call(x_in, dy_in, gain, w_q, wkv, wo)

        n_dev = mesh.shape['cp']
        pair_perm = [(d, d ^ 1) for d in range(n_dev)]
        dwo_recv, dwq_recv = lax.ppermute((dwo_own, dwq_own), 'cp', pair_perm)

        x2 = x_in.reshape(rows, dm)
        dx, dg = dx_call(dq_own.reshape(rows, -1), wq, wkv, x2, dy_in.reshape(rows, dm), gain)
        dg = jnp.sum(dg, axis=0)
        dg1 = lax.ppermute(dg, 'cp', pair_perm)
        dg2 = lax.ppermute(dg, 'cp', [(d, d ^ 2) for d in range(n_dev)])
        dg3 = lax.ppermute(dg, 'cp', [(d, d ^ 3) for d in range(n_dev)])
        y, d_wo, d_wq, d_wk, d_wv = y_call(core, o_own.reshape(rows, -1), wo, x2, dwo_own, dwo_recv, dwq_own, dwq_recv,
                                           n_heads, hd)
        y, dg, dg1, dg2, dg3 = lax.optimization_barrier((y, dg, dg1, dg2, dg3))
        d_gain = (dg + dg1) + (dg2 + dg3)
        return (y.reshape(x_in.shape), dx.reshape(x_in.shape), d_gain, d_wq, d_wk, d_wv, d_wo.reshape(n_heads, hd, dm))

    act_spec = P('dp', 'cp', None)
    mat_spec = P(None, None, None)
    grad_spec = P('dp', None, None)
    return jax.shard_map(device_fn, mesh=mesh,
                         in_specs=(act_spec, act_spec, P(None), mat_spec, mat_spec, mat_spec, mat_spec),
                         out_specs=(act_spec, act_spec, P('dp'), grad_spec, grad_spec, grad_spec, grad_spec),
                         check_vma=False)
```

```python
import functools

import jax
import jax.numpy as jnp
from jax import lax
from jax.experimental import pallas as pl
from jax.experimental.pallas import tpu as pltpu
from jax.sharding import PartitionSpec as P

EPS = 1e-6
F32 = jnp.float32
BF16 = jnp.bfloat16
LOG2E = 1.4426950408889634
MESH = pl.DeviceIdType.MESH
CROSS_AHEAD = 4
PAIR_AHEAD = 2


def dot_nn(a, b):
    return lax.dot_general(a, b, (((1,), (0,)), ((), ())), preferred_element_type=F32)


def dot_nt(a, b):
    return lax.dot_general(a, b, (((1,), (1,)), ((), ())), preferred_element_type=F32)


def group_kernel(x, dy, gain, w_q, wkv, wo, gx, gy, dwo, dwq, oo, dqo, xn, wq,
                 xb, yb, gain_v, w_in, w_f32, wq_v, wo_v, acc_o, acc_q, q_s, do_s, k_s, v_s, kt_s, vt_s,
                 ot_s, dqt_s, dk_acc, dv_acc, o_n, dq_n,
                 cs, cr, ds, dr, fs, fr, lsem, wsem, osem, psend, precv, fsem, nsem, rsem):
    n_seq, blk, dm = x.shape
    seq = 4 * blk
    n_heads, _, hd = q_s.shape
    qw = n_heads * hd
    half = 2 * blk
    tile = 256
    n_tiles = seq // tile
    c2 = LOG2E * hd ** -0.5
    scale = hd ** -0.5

    me = lax.axis_index('cp')
    core = me % 2
    chip = me // 2
    pair = chip * 2 + (1 - core)
    across = (1 - chip) * 2 + core
    diag = (1 - chip) * 2 + (1 - core)
    src_of = (xn, dy)
    land_of = (gx, gy)
    vmem_of = (xb, yb)

    def cross_copy(t, s):
        return pltpu.make_async_remote_copy(src_of[t].at[s], land_of[t].at[me, s], cs.at[t, s], cr.at[t, s],
                                            device_id={'cp': across}, device_id_type=MESH)

    def cross_arrival(t, s):
        return pltpu.make_async_remote_copy(src_of[t].at[s], land_of[t].at[across, s], cs.at[t, s], cr.at[t, s],
                                            device_id={'cp': across}, device_id_type=MESH)

    def pair_copy(t, s):
        return pltpu.make_async_remote_copy(src_of[t].at[s], land_of[t].at[me, s], ds.at[t, s], dr.at[t, s],
                                            device_id={'cp': pair}, device_id_type=MESH)

    def pair_arrival(t, s):
        return pltpu.make_async_remote_copy(src_of[t].at[s], land_of[t].at[pair, s], ds.at[t, s], dr.at[t, s],
                                            device_id={'cp': pair}, device_id_type=MESH)

    def fwd_copy(t, s):
        return pltpu.make_async_remote_copy(land_of[t].at[across, s], land_of[t].at[across, s], fs.at[t, s], fr.at[t, s],
                                            device_id={'cp': pair}, device_id_type=MESH)

    def fwd_arrival(t, s):
        return pltpu.make_async_remote_copy(land_of[t].at[across, s], land_of[t].at[diag, s], fs.at[t, s], fr.at[t, s],
                                            device_id={'cp': pair}, device_id_type=MESH)

    def rows_of(b):
        return pl.ds(pl.multiple_of(b * blk, 64), blk)

    def load_own(t, s):
        return pltpu.make_async_copy(src_of[t].at[s], vmem_of[t].at[s % 2, rows_of(me)], lsem.at[t, 0])

    def load_from(t, s, b, j):
        return pltpu.make_async_copy(land_of[t].at[b, s], vmem_of[t].at[s % 2, rows_of(b)], lsem.at[t, j])

    kvw = 2 * hd

    def out_parts(s, g):
        q_cols = pl.ds(pl.multiple_of(g * qw, 128), qw)
        kv_cols = pl.ds(pl.multiple_of(2 * qw + g * kvw, 128), kvw)
        return ((o_n, slice(0, qw), oo.at[s, :, q_cols]),
                (dq_n, slice(0, qw), dqo.at[s, :, q_cols]),
                (dq_n, slice(qw, qw + kvw), dqo.at[s, :, kv_cols]))

    def pair_send(idx, s, buf, cols, dst):
        rows = pl.ds(pl.multiple_of((1 - core) * blk, 64), blk)
        return pltpu.make_async_remote_copy(buf.at[rows, cols], dst, psend.at[idx], precv.at[idx, s],
                                            device_id={'cp': pair}, device_id_type=MESH)

    def out_copies(s):
        rows = pl.ds(pl.multiple_of(core * blk, 64), blk)
        return [(pltpu.make_async_copy(buf.at[rows, cols], dst, osem.at[idx]), pair_send(idx, s, buf, cols, dst))
                for idx, (buf, cols, dst) in enumerate(out_parts(s, core))]

    def out_arrivals(s):
        return [pair_send(idx, s, buf, cols, dst) for idx, (buf, cols, dst) in enumerate(out_parts(s, 1 - core))]

    weight_loads = [
        pltpu.make_async_copy(gain, gain_v, wsem.at[0]),
        pltpu.make_async_copy(wq.at[:, pl.ds(pl.multiple_of(core * qw, 128), qw)], wq_v.at[:, 0:qw], wsem.at[1]),
        pltpu.make_async_copy(wkv.at[:, pl.ds(pl.multiple_of(core * kvw, 128), kvw)], wq_v.at[:, qw:qw + kvw], wsem.at[2]),
        pltpu.make_async_copy(wo.at[pl.ds(pl.multiple_of(core * qw, 128), qw)], wo_v, wsem.at[3]),
    ]

    def norm_in(s):
        return pltpu.make_async_copy(x.at[s], yb.at[1, pl.ds(pl.multiple_of((s % 2) * blk, 64), blk)], nsem.at[0, s % 2])

    def norm_out(s):
        return pltpu.make_async_copy(xb.at[1, pl.ds(pl.multiple_of((s % 2) * blk, 64), blk)], xn.at[s], nsem.at[1, s % 2])

    n_wrows = w_in.shape[1]
    n_wsteps = dm // n_wrows
    stage0 = half

    def relay_in(c):
        return pltpu.make_async_copy(w_q.at[pl.ds(pl.multiple_of(c * n_wrows, n_wrows), n_wrows)], w_in.at[c % 2],
                                     rsem.at[0, c % 2])

    def relay_out(c):
        return pltpu.make_async_copy(xb.at[1, pl.ds(pl.multiple_of(stage0 + (c % 2) * n_wrows, n_wrows), n_wrows)],
                                     wq.at[pl.ds(pl.multiple_of(c * n_wrows, n_wrows), n_wrows)], rsem.at[1, c % 2])

    def relay_step(c, carry):
        @pl.when(c + 1 < n_wsteps)
        def _():
            relay_in(c + 1).start()
        relay_in(c).wait()

        @pl.when(c > 1)
        def _():
            relay_out(c - 2).wait()
        w_f32[...] = w_in[c % 2].astype(F32)
        rows = pl.ds(pl.multiple_of(stage0 + (c % 2) * n_wrows, n_wrows), n_wrows)
        for h in range(2 * n_heads):
            xb[1, rows, h * hd:(h + 1) * hd] = w_f32[:, h, :].astype(BF16)
        relay_out(c).start()
        return carry

    norm_in(0).start()
    relay_in(0).start()
    for copy in (weight_loads[0], weight_loads[2], weight_loads[3]):
        copy.start()

    barrier = pltpu.get_barrier_semaphore()
    for peer in (pair, across):
        pl.semaphore_signal(barrier, inc=1, device_id={'cp': peer}, device_id_type=MESH)
    pl.semaphore_wait(barrier, 2)

    cross_copy(1, 0).start()
    pair_copy(1, 0).start()
    load_own(1, 0).start()
    weight_loads[0].wait()

    def send_normed(s):
        norm_out(s).wait()

        @pl.when(s < CROSS_AHEAD)
        def _():
            cross_copy(0, s).start()

        @pl.when(s + 1 < CROSS_AHEAD)
        def _():
            cross_copy(1, s + 1).start()

        @pl.when(s < PAIR_AHEAD)
        def _():
            pair_copy(0, s).start()

        @pl.when(s + 1 < PAIR_AHEAD)
        def _():
            pair_copy(1, s + 1).start()

    def norm_step(s, carry):
        @pl.when(s + 1 < n_seq)
        def _():
            norm_in(s + 1).start()
        norm_in(s).wait()
        base = (s % 2) * blk
        for c in range(blk // 48):
            rows = pl.ds(pl.multiple_of(base + c * 48, 16), 48)
            xf = yb[1, rows, :].astype(F32)
            r = lax.rsqrt(jnp.mean(xf * xf, axis=-1, keepdims=True) + EPS)
            xb[1, rows, :] = (xf * r * gain_v[...]).astype(BF16)
        norm_out(s).start()

        @pl.when(s > 0)
        def _():
            send_normed(s - 1)
        return carry

    lax.fori_loop(0, n_seq, norm_step, 0)
    send_normed(n_seq - 1)
    load_own(0, 0).start()
    lax.fori_loop(0, n_wsteps, relay_step, 0)
    relay_out(n_wsteps - 2).wait()
    relay_out(n_wsteps - 1).wait()
    weight_loads[1].start()
    acc_o[...] = jnp.zeros_like(acc_o)
    acc_q[...] = jnp.zeros_like(acc_q)
    for t in range(2):
        pair_arrival(t, 0).wait_recv()
        load_from(t, 0, pair, 1).start()
    for copy in weight_loads[1:]:
        copy.wait()

    def project_x(slot, r0):
        rows = pl.ds(pl.multiple_of(r0, 128), half)
        for n in range((qw + 2 * hd) // tile):
            res = dot_nn(xb[slot, rows, :], wq_v[:, n * tile:(n + 1) * tile]).astype(BF16)
            for part in range(tile // hd):
                col = n * tile + part * hd
                piece = res[:, part * hd:(part + 1) * hd]
                if col < qw:
                    q_s[col // hd, rows, :] = piece
                elif col == qw:
                    k_s[rows, :] = piece
                else:
                    v_s[rows, :] = piece

    def project_dy(slot, r0):
        rows = pl.ds(pl.multiple_of(r0, 128), half)
        for n in range(qw // tile):
            res = dot_nt(yb[slot, rows, :], wo_v[n * tile:(n + 1) * tile, :]).astype(BF16)
            for part in range(tile // hd):
                do_s[(n * tile + part * hd) // hd, rows, :] = res[:, part * hd:(part + 1) * hd]

    def heads():
        units = [(h, i) for h in range(n_heads) for i in range(n_tiles)]
        state = {}

        def score(u):
            h, i = units[u]
            nk = (i + 1) * tile
            qi = q_s[h, i * tile:(i + 1) * tile, :]
            doi = do_s[h, i * tile:(i + 1) * tile, :]
            state[u] = [dot_nt(k_s[0:nk, :], qi), dot_nt(v_s[0:nk, :], doi)]

        def attend(u):
            h, i = units[u]
            nk = (i + 1) * tile
            st, dpt = state[u]
            key_pos = lax.broadcasted_iota(jnp.int32, (tile, tile), 0)
            qry_pos = lax.broadcasted_iota(jnp.int32, (tile, tile), 1)
            edge = jnp.where(key_pos <= qry_pos, st[nk - tile:], -jnp.inf)
            st = edge if i == 0 else jnp.concatenate([st[:nk - tile], edge], axis=0)
            mx = jnp.max(st, axis=0, keepdims=True)
            p = jnp.exp2(st * c2 - mx * c2)
            inv_l = 1.0 / jnp.sum(p, axis=0, keepdims=True)
            ot = (dot_nn(vt_s[:, 0:nk], p.astype(BF16)) * inv_l).astype(BF16)
            ot_s[h * hd:(h + 1) * hd, i * tile:(i + 1) * tile] = ot
            state[u] = [p, inv_l, ot, dpt]

        def grads(u):
            h, i = units[u]
            nk = (i + 1) * tile
            p, inv_l, ot, dpt = state.pop(u)
            qi = q_s[h, i * tile:(i + 1) * tile, :]
            doi = do_s[h, i * tile:(i + 1) * tile, :]
            delta = jnp.sum(doi.astype(F32).T * ot.astype(F32), axis=0, keepdims=True)
            pn = p * inv_l
            dst = (pn * (dpt - delta) * scale).astype(BF16)
            dv_acc[0:nk, :] += dot_nn(pn.astype(BF16), doi)
            dk_acc[0:nk, :] += dot_nn(dst, qi)
            dqt_s[h * hd:(h + 1) * hd, i * tile:(i + 1) * tile] = dot_nn(kt_s[:, 0:nk], dst).astype(BF16)

        for t in range(-2, len(units)):
            if t + 2 < len(units):
                score(t + 2)
            if 0 <= t + 1 < len(units):
                attend(t + 1)
            if t >= 0:
                grads(t)
        own_cols = pl.ds(pl.multiple_of(chip * half, 128), half)
        for h in range(n_heads):
            o_n[:, h * hd:(h + 1) * hd] = ot_s[h * hd:(h + 1) * hd, own_cols].T
            dq_n[:, h * hd:(h + 1) * hd] = dqt_s[h * hd:(h + 1) * hd, own_cols].T

    def wide(n):
        return pl.ds(pl.multiple_of(n * 2 * tile, 2 * tile), 2 * tile)

    def seq_step(s, carry):
        slot = s % 2
        prev = (s + 1) % 2
        live = s < n_seq
        near = chip * half
        far = (1 - chip) * half

        @pl.when(s + CROSS_AHEAD < n_seq)
        def _():
            for t in range(2):
                cross_copy(t, s + CROSS_AHEAD).start()

        @pl.when(s + PAIR_AHEAD < n_seq)
        def _():
            for t in range(2):
                pair_copy(t, s + PAIR_AHEAD).start()

        @pl.when(live)
        def _():
            cross_arrival(0, s).wait_recv()
            fwd_copy(0, s).start()
            load_from(0, s, across, 2).start()
            for t in range(2):
                load_own(t, s).wait()
                load_from(t, s, pair, 1).wait()
            project_x(slot, near)
            project_dy(slot, near)
            fwd_arrival(0, s).wait_recv()
            load_from(0, s, diag, 3).start()
            load_from(0, s, across, 2).wait()
            load_from(0, s, diag, 3).wait()
            project_x(slot, far)

        @pl.when(s > 0)
        def _():
            def dwo_step(n, c):
                acc_o[:, wide(n)] += dot_nn(ot_s[...], yb[prev, :, wide(n)])
                return c

            lax.fori_loop(0, dm // (2 * tile), dwo_step, 0)

        @pl.when(live)
        def _():
            cross_arrival(1, s).wait_recv()
            fwd_copy(1, s).start()
            load_from(1, s, across, 2).start()

        @pl.when(s == n_seq)
        def _():
            flush_o.start()

        @pl.when(s > 0)
        def _():
            def dwq_step(n, c):
                acc_q[:, wide(n)] += dot_nn(dqt_s[...], xb[prev, :, wide(n)])

                @pl.when(s == n_seq)
                def _():
                    flush_q(n).start()
                return c

            lax.fori_loop(0, dm // (2 * tile), dwq_step, 0)

        @pl.when(live)
        def _():
            fwd_arrival(1, s).wait_recv()
            load_from(1, s, diag, 3).start()

            @pl.when(s + 1 < n_seq)
            def _():
                for t in range(2):
                    load_own(t, s + 1).start()
                    pair_arrival(t, s + 1).wait_recv()
                    load_from(t, s + 1, pair, 1).start()

            @pl.when(s > 0)
            def _():
                for local, remote in out_copies(s - 1):
                    local.wait()
                    remote.wait_send()
            load_from(1, s, across, 2).wait()
            load_from(1, s, diag, 3).wait()
            kt_s[...] = k_s[...].T
            vt_s[...] = v_s[...].T
            dk_acc[...] = jnp.zeros_like(dk_acc)
            dv_acc[...] = jnp.zeros_like(dv_acc)
            project_dy(slot, far)
            heads()
            near_rows = pl.ds(pl.multiple_of(near, 128), half)
            for idx, acc in enumerate((dk_acc, dv_acc)):
                lo = qw + idx * hd
                dqt_s[lo:lo + hd, :] = acc[...].T.astype(BF16)
                dq_n[:, lo:lo + hd] = acc[near_rows, :].astype(BF16)
            for local, remote in out_copies(s):
                local.start()
                remote.start()
        return carry

    flush_o = pltpu.make_async_copy(acc_o, dwo, fsem.at[0])

    def flush_q(n):
        return pltpu.make_async_copy(acc_q.at[:, wide(n)], dwq.at[:, wide(n)], fsem.at[1 + n])

    lax.fori_loop(0, n_seq + 1, seq_step, 0)

    for local, remote in out_copies(n_seq - 1):
        local.wait()
        remote.wait_send()

    def drain(s, carry):
        for t in range(2):
            cross_copy(t, s).wait_send()
            pair_copy(t, s).wait_send()
            fwd_copy(t, s).wait_send()
        for arrival in out_arrivals(s):
            arrival.wait_recv()
        return carry

    lax.fori_loop(0, n_seq, drain, 0)
    flush_o.wait()
    for n in range(dm // (2 * tile)):
        flush_q(n).wait()


def group_call(x_in, dy_in, gain, w_q, wkv, wo):
    n_seq, blk, dm = x_in.shape
    seq = 4 * blk
    n_heads, hd = w_q.shape[1] // 2, w_q.shape[2]
    qw = n_heads * hd
    kw = qw + 2 * hd
    any_spec = pl.BlockSpec(memory_space=pl.ANY)
    dma = pltpu.SemaphoreType.DMA
    rows = n_seq * seq
    flops = 2 * rows * dm * (2 * kw + 2 * qw) + 12 * n_seq * n_heads * seq * seq * hd
    return pl.pallas_call(
        group_kernel,
        out_shape=(
            jax.ShapeDtypeStruct((4, n_seq, blk, dm), BF16),
            jax.ShapeDtypeStruct((4, n_seq, blk, dm), BF16),
            jax.ShapeDtypeStruct((qw, dm), F32),
            jax.ShapeDtypeStruct((kw, dm), F32),
            jax.ShapeDtypeStruct((n_seq, blk, 2 * qw), BF16),
            jax.ShapeDtypeStruct((n_seq, blk, 2 * kw), BF16),
            jax.ShapeDtypeStruct((n_seq, blk, dm), BF16),
            jax.ShapeDtypeStruct((dm, 2 * qw), BF16),
        ),
        in_specs=[any_spec] * 6,
        out_specs=(any_spec,) * 8,
        scratch_shapes=[
            pltpu.VMEM((2, seq, dm), BF16), pltpu.VMEM((2, seq, dm), BF16), pltpu.VMEM((1, dm), F32),
            pltpu.VMEM((2, 64, 2 * n_heads, hd), BF16), pltpu.VMEM((64, 2 * n_heads, hd), F32),
            pltpu.VMEM((dm, kw), BF16), pltpu.VMEM((qw, dm), BF16),
            pltpu.VMEM((qw, dm), F32), pltpu.VMEM((kw, dm), F32),
            pltpu.VMEM((n_heads, seq, hd), BF16), pltpu.VMEM((n_heads, seq, hd), BF16),
            pltpu.VMEM((seq, hd), BF16), pltpu.VMEM((seq, hd), BF16),
            pltpu.VMEM((hd, seq), BF16), pltpu.VMEM((hd, seq), BF16),
            pltpu.VMEM((qw, seq), BF16), pltpu.VMEM((kw, seq), BF16),
            pltpu.VMEM((seq, hd), F32), pltpu.VMEM((seq, hd), F32),
            pltpu.VMEM((2 * blk, qw), BF16), pltpu.VMEM((2 * blk, kw), BF16),
            dma((2, n_seq)), dma((2, n_seq)), dma((2, n_seq)), dma((2, n_seq)), dma((2, n_seq)), dma((2, n_seq)),
            dma((2, 4)), dma((4,)), dma((3,)), dma((3,)), dma((3, n_seq)), dma((1 + dm // 512,)), dma((2, 2)), dma((2, 2)),
        ],
        cost_estimate=pl.CostEstimate(flops=flops, bytes_accessed=400_000_000, transcendentals=0),
        compiler_params=pltpu.CompilerParams(collective_id=0, has_side_effects=True, vmem_limit_bytes=67_000_000),
    )(x_in, dy_in, gain, w_q, wkv, wo)


def dx_kernel(dq, wq, wkv, x, dy, gain, dx, dg, dn, w_all, wsem):
    i = pl.program_id(0)
    n_tiles = pl.num_programs(0) - 1
    tm, dm = x.shape
    parts = 4
    cw = dm // parts
    cr = tm // parts

    def matmul(n):
        cols = pl.ds(pl.multiple_of(n * cw, cw), cw)
        dn[i % 2, :, cols] = dot_nt(dq[...], w_all[cols, :])

    def finish(n):
        rows = pl.ds(pl.multiple_of(n * cr, 16), cr)
        xf = x[rows, :].astype(F32)
        r = lax.rsqrt(jnp.mean(xf * xf, axis=-1, keepdims=True) + EPS)
        u = xf * r
        d = dn[(i + 1) % 2, rows, :]
        du = d * u
        dg[...] += jnp.sum(du.reshape(cr // 8, 8, dm), axis=0)
        g = gain[...]
        mean_eu = jnp.mean(du * g, axis=-1, keepdims=True)
        dx[rows, :] = (dy[rows, :].astype(F32) + r * (d * g - u * mean_eu)).astype(BF16)

    @pl.when(i == 0)
    def _():
        qw = wq.shape[1]

        def loads(n):
            rows = pl.ds(pl.multiple_of(n * cw, cw), cw)
            return (pltpu.make_async_copy(wq.at[rows], w_all.at[rows, 0:qw], wsem.at[0, n]),
                    pltpu.make_async_copy(wkv.at[rows], w_all.at[rows, qw:], wsem.at[1, n]))

        for n in range(parts):
            for copy in loads(n):
                copy.start()
        dg[...] = jnp.zeros_like(dg)

        @pl.loop(0, parts)
        def _(n):
            for copy in loads(n):
                copy.wait()
            matmul(n)

    @pl.when(jnp.logical_and(i > 0, i < n_tiles))
    def _():
        @pl.loop(0, parts)
        def _(n):
            finish(n)
            matmul(n)

    @pl.when(i == n_tiles)
    def _():
        @pl.loop(0, parts)
        def _(n):
            finish(n)


def dx_call(dq, wq, wkv, x, dy, gain):
    rows, dm = x.shape
    kw = dq.shape[1]
    tm = 384
    n_tiles = rows // tm
    late = lambda i: (jnp.maximum(i - 1, 0), 0)
    any_spec = pl.BlockSpec(memory_space=pl.ANY)
    return pl.pallas_call(
        dx_kernel,
        grid=(n_tiles + 1,),
        out_shape=(jax.ShapeDtypeStruct((rows, dm), BF16), jax.ShapeDtypeStruct((8, dm), F32)),
        in_specs=[pl.BlockSpec((tm, kw), lambda i: (jnp.minimum(i, n_tiles - 1), 0)),
                  any_spec, any_spec,
                  pl.BlockSpec((tm, dm), late), pl.BlockSpec((tm, dm), late),
                  pl.BlockSpec((1, dm), lambda i: (0, 0))],
        out_specs=(pl.BlockSpec((tm, dm), late), pl.BlockSpec((8, dm), lambda i: (0, 0))),
        scratch_shapes=[pltpu.VMEM((2, tm, dm), F32), pltpu.VMEM((dm, kw), BF16), pltpu.SemaphoreType.DMA((2, 4))],
        cost_estimate=pl.CostEstimate(flops=2 * rows * dm * kw, bytes_accessed=50_000_000, transcendentals=0),
        compiler_params=pltpu.CompilerParams(vmem_limit_bytes=60_000_000),
    )(dq, wq, wkv, x, dy, gain)


def y_kernel(core_ref, o, wo, x, own_o, recv_o, own_q, recv_q, y, d_wo, d_wq, d_wk, d_wv, wo_v, wsem):
    i = pl.program_id(0)
    core = core_ref[0]
    n_heads, hd = d_wq.shape[1], d_wq.shape[2]
    n_group = n_heads // 2
    load = pltpu.make_async_copy(wo, wo_v, wsem)

    def place():
        mine = i // (pl.num_programs(0) // 2) == core
        d_wo[...] = jnp.where(mine, own_o[...], recv_o[...])
        for g in range(2):
            own = core == g
            for h in range(n_group + 2):
                rows = pl.ds(h * hd, hd)
                val = jnp.where(own, own_q[rows, :], recv_q[rows, :]).T
                if h < n_group:
                    d_wq[:, g * n_group + h, :] = val
                elif h == n_group:
                    d_wk[:, g, :] = val
                else:
                    d_wv[:, g, :] = val

    def project():
        y[...] = (x[...].astype(F32) + dot_nn(o[...], wo_v[...])).astype(BF16)

    @pl.when(i == 0)
    def _():
        load.start()
        place()
        load.wait()
        project()

    @pl.when(i > 0)
    def _():
        project()
        place()


def y_call(core, o, wo, x, own_o, recv_o, own_q, recv_q, n_heads, hd):
    rows, dm = x.shape
    qw2 = o.shape[1]
    kw = own_q.shape[0]
    steps = 8
    tm = rows // steps
    tw = qw2 // steps
    tn = dm // steps
    hs = steps // 2
    grid_spec = pltpu.PrefetchScalarGridSpec(
        num_scalar_prefetch=1,
        grid=(steps,),
        in_specs=[pl.BlockSpec((tm, qw2), lambda i, c: (i, 0)),
                  pl.BlockSpec(memory_space=pl.ANY),
                  pl.BlockSpec((tm, dm), lambda i, c: (i, 0)),
                  pl.BlockSpec((tw, dm), lambda i, c: (jnp.clip(i - hs * c[0], 0, hs - 1), 0)),
                  pl.BlockSpec((tw, dm), lambda i, c: (jnp.clip(i - hs * (1 - c[0]), 0, hs - 1), 0)),
                  pl.BlockSpec((kw, tn), lambda i, c: (0, i)),
                  pl.BlockSpec((kw, tn), lambda i, c: (0, i))],
        out_specs=(pl.BlockSpec((tm, dm), lambda i, c: (i, 0)),
                   pl.BlockSpec((tw, dm), lambda i, c: (i, 0)),
                   pl.BlockSpec((tn, n_heads, hd), lambda i, c: (i, 0, 0)),
                   pl.BlockSpec((tn, 2, hd), lambda i, c: (i, 0, 0)),
                   pl.BlockSpec((tn, 2, hd), lambda i, c: (i, 0, 0))),
        scratch_shapes=[pltpu.VMEM((qw2, dm), BF16), pltpu.SemaphoreType.DMA])
    return pl.pallas_call(
        y_kernel,
        grid_spec=grid_spec,
        out_shape=(jax.ShapeDtypeStruct((rows, dm), BF16), jax.ShapeDtypeStruct((qw2, dm), F32),
                   jax.ShapeDtypeStruct((dm, n_heads, hd), F32),
                   jax.ShapeDtypeStruct((dm, 2, hd), F32), jax.ShapeDtypeStruct((dm, 2, hd), F32)),
        cost_estimate=pl.CostEstimate(flops=2 * rows * dm * qw2, bytes_accessed=110_000_000, transcendentals=0),
        compiler_params=pltpu.CompilerParams(vmem_limit_bytes=60_000_000),
    )(core, o, wo, x, own_o, recv_o, own_q, recv_q)


def solution(mesh):
    def device_fn(x_in, dy_in, norm_gain, w_q, w_k, w_v, w_o):
        n_batch, blk, dm = x_in.shape
        n_heads, hd = w_q.shape[1], w_q.shape[2]
        rows = n_batch * blk
        qw = n_heads * hd // 2
        core = (lax.axis_index('cp') % 2).astype(jnp.int32).reshape(1)
        gain = norm_gain.astype(F32).reshape(1, dm)
        wkv = jnp.concatenate([w_k, w_v], axis=2).reshape(dm, 4 * hd)
        wo = w_o.reshape(n_heads * hd, dm)

        _, _, dwo_own, dwq_own, o_own, dq_own, _, wq = group_call(x_in, dy_in, gain, w_q, wkv, wo)

        n_dev = mesh.shape['cp']
        pair_perm = [(d, d ^ 1) for d in range(n_dev)]
        dwo_recv, dwq_recv = lax.ppermute((dwo_own, dwq_own), 'cp', pair_perm)

        x2 = x_in.reshape(rows, dm)
        dx, dg = dx_call(dq_own.reshape(rows, -1), wq, wkv, x2, dy_in.reshape(rows, dm), gain)
        dg = jnp.sum(dg, axis=0)
        dg1 = lax.ppermute(dg, 'cp', pair_perm)
        dg2 = lax.ppermute(dg, 'cp', [(d, d ^ 2) for d in range(n_dev)])
        dg3 = lax.ppermute(dg, 'cp', [(d, d ^ 3) for d in range(n_dev)])
        y, d_wo, d_wq, d_wk, d_wv = y_call(core, o_own.reshape(rows, -1), wo, x2, dwo_own, dwo_recv, dwq_own, dwq_recv,
                                           n_heads, hd)
        y, dg, dg1, dg2, dg3 = lax.optimization_barrier((y, dg, dg1, dg2, dg3))
        d_gain = (dg + dg1) + (dg2 + dg3)
        return (y.reshape(x_in.shape), dx.reshape(x_in.shape), d_gain, d_wq, d_wk, d_wv, d_wo.reshape(n_heads, hd, dm))

    act_spec = P('dp', 'cp', None)
    mat_spec = P(None, None, None)
    grad_spec = P('dp', None, None)
    return jax.shard_map(device_fn, mesh=mesh,
                         in_specs=(act_spec, act_spec, P(None), mat_spec, mat_spec, mat_spec, mat_spec),
                         out_specs=(act_spec, act_spec, P('dp'), grad_spec, grad_spec, grad_spec, grad_spec),
                         check_vma=False)
```
